256 devices in a mesh: row: 8 (over y, x_hi), col: 32 (over z, x_lo, core).
Axes of the slice: x: 4 (x_hi: 2, x_lo: 2; x = x_hi * 2 + x_lo), y: 4, z: 8, core: 2. Of those that a mesh axis runs over, the one named last changes fastest.
Arguments:
- pair: float32 [512, 512, 128], P('row', 'col'), may hold values from -6 to 6
- in_gain: float32 [2, 128], replicated, may hold values from 1 to 4
- in_bias: float32 [2, 128], replicated, may hold values from -1.5 to 1.5
- proj_weight: bfloat16 [2, 128, 640], replicated, may hold values from -0.5 to 0.5
- proj_bias: float32 [2, 640], replicated, may hold values from -1.5 to 1.5
- mid_gain: float32 [2, 128], replicated, may hold values from 0.5 to 2
- mid_bias: float32 [2, 128], replicated, may hold values from -3 to 3
- out_weight: bfloat16 [2, 128, 128], replicated, may hold values from -0.5 to 0.5
- out_bias: float32 [2, 128], replicated, may hold values from -3 to 3
Outputs:
- updated: float32 [512, 512, 128], P('row', 'col')
The draws below stay inside these ranges and needn't reach their ends.
All inputs are finite; a program needn't handle non-finite values.
Results may differ from the reference program's by a relative error of at most 0.015.
Values may be sent and summed in bfloat16 or wider, within the bound.
A program may use at most 128 MiB of HBM per device.

```python
import math
import jax
import jax.numpy as jnp
from jax import lax

C = 128
HID = 128
N = 512


def shard_levels(rng, shape, shards, smallest, top_value):
    def one(dim, blocks):
        heights = jax.random.uniform(jax.random.fold_in(jax.random.fold_in(rng, 6), dim), (blocks,), jnp.float32, smallest / len(shards), top_value / len(shards))
        return jnp.repeat(jnp.exp(heights), shape[dim] // blocks).reshape((-1,) + (1,) * (len(shape) - dim - 1))

    level = one(*shards[0])
    for cut in shards[1:]:
        level = level * one(*cut)
    return level


def noise(key, extent, scale, limit, cuts=(), held_as=jnp.bfloat16):
    drawn = jax.random.normal(key, extent, jnp.float32) * scale
    if len(cuts) > 0:
        drawn = shard_levels(key, extent, cuts, -0.22, 0.18) * drawn
    return jnp.clip(drawn, min=-limit, max=limit).astype(held_as)


def setup_inputs(seed: int = 0) -> dict:
    arg_keys = jax.random.split(jax.random.key(seed), 10)
    return {
        "pair": noise(arg_keys[0], (N, N, C), 1.0, 6.0, ((0, 8), (1, 32)), jnp.float32),
        "in_gain": jnp.clip(jnp.exp(jax.random.uniform(arg_keys[1], (2, C), jnp.float32, math.log(1.0), math.log(4.0))), 1.0, 4.0),
        "in_bias": noise(arg_keys[2], (2, C), 0.25, 1.5, (), jnp.float32),
        "proj_weight": noise(arg_keys[3], (2, C, 4 * HID + C), C ** -0.5, 0.5),
        "proj_bias": noise(arg_keys[4], (2, 4 * HID + C), 0.25, 1.5, (), jnp.float32),
        "mid_gain": jnp.clip(jnp.exp(jax.random.uniform(arg_keys[5], (2, HID), jnp.float32, math.log(0.5), math.log(2.0))), 0.5, 2.0),
        "mid_bias": noise(arg_keys[6], (2, HID), 0.5, 3.0, (), jnp.float32),
        "out_weight": noise(arg_keys[7], (2, HID, C), HID ** -0.5, 0.5),
        "out_bias": noise(arg_keys[8], (2, C), 0.5, 3.0, (), jnp.float32),
    }


def layer_norm(values, gain, offset):
    mean = lax.optimization_barrier(jnp.mean(values, -1, keepdims=True))
    centred = values - mean
    variance = lax.optimization_barrier(jnp.mean(centred * centred, -1, keepdims=True))
    return centred * lax.rsqrt(variance + 1e-05) * gain + offset

def reference(pair, in_gain, in_bias, proj_weight, proj_bias, mid_gain, mid_bias, out_weight, out_bias):
    hidden = out_weight.shape[1]
    state = pair
    for update in range(2):
        normed = layer_norm(state, in_gain[update], in_bias[update]).astype(jnp.bfloat16)
        proj = jnp.dot(normed, proj_weight[update], preferred_element_type=jnp.float32) + proj_bias[update]
        left = (jax.nn.sigmoid(proj[..., hidden:2 * hidden]) * proj[..., 0:hidden]).astype(jnp.bfloat16)
        right = (jax.nn.sigmoid(proj[..., 3 * hidden:4 * hidden]) * proj[..., 2 * hidden:3 * hidden]).astype(jnp.bfloat16)
        gate = jax.nn.sigmoid(proj[..., 4 * hidden:])
        if update == 0:
            mixed = jnp.einsum('ikc,jkc->ijc', left.astype(jnp.float32), right.astype(jnp.float32))
        else:
            mixed = jnp.einsum('kic,kjc->ijc', left.astype(jnp.float32), right.astype(jnp.float32))
        middle = layer_norm(mixed, mid_gain[update], mid_bias[update]).astype(jnp.bfloat16)
        outcome = jnp.dot(middle, out_weight[update], preferred_element_type=jnp.float32) + out_bias[update]
        state = state + gate * outcome
    return state
```

```python
import functools

import jax
import jax.numpy as jnp
from jax import lax
from jax.experimental import pallas as pl
from jax.experimental.pallas import tpu as pltpu
from jax.sharding import PartitionSpec as P

MESH = pl.DeviceIdType.MESH
F32 = jnp.float32
BF16 = jnp.bfloat16
EPS = 1e-05


def norm_rows(values, gain, offset):
    mean = jnp.mean(values, -1, keepdims=True)
    centred = values - mean
    variance = jnp.mean(centred * centred, -1, keepdims=True)
    return centred * lax.rsqrt(variance + EPS) * gain + offset


def kernel(
    pair_ref, in_gain, in_bias, proj_w, proj_b, mid_gain, mid_bias, out_w, out_b,
    out_ref,
    w_t, bias_t, mgain_t, mbias_t,
    state, gates, tmp_l, tmp_r,
    send_l, send_r, send_m, recv_l, recv_r, recv_m,
    a_l0, a_l1, a_r, mixed,
    sems_send, sems_recv, sem_enter,
):
    row = lax.axis_index("row")
    col = lax.axis_index("col")
    y, xh = lax.div(row, 2), lax.rem(row, 2)
    z, low = lax.div(col, 4), lax.rem(col, 4)
    xl, core = lax.div(low, 2), lax.rem(low, 2)
    x = xh * 2 + xl
    chip = (y * 4 + x) * 8 + z
    partner = col + 1 - 2 * core
    half_r = lax.div(y, 2)
    half_z = lax.div(z, 4)

    barrier = pltpu.get_barrier_semaphore()

    def greet_row(t, _):
        pl.semaphore_signal(
            barrier, inc=1, device_id=(lax.rem(row + t, 8), col), device_id_type=MESH
        )
        return 0

    def greet_col(t, _):
        pl.semaphore_signal(
            barrier, inc=1, device_id=(row, lax.rem(col + t, 32)), device_id_type=MESH
        )
        return 0

    lax.fori_loop(1, 8, greet_row, 0)
    lax.fori_loop(1, 32, greet_col, 0)

    def prepare(u):
        w_t[u] = jnp.transpose(proj_w[u, :, 0:512].astype(F32)).astype(BF16)
        bias_t[u] = jnp.transpose(
            jnp.broadcast_to(proj_b[u : u + 1, 0:512], (128, 512))
        )
        mgain_t[u] = jnp.transpose(jnp.broadcast_to(mid_gain[u : u + 1, :], (128, 128)))
        mbias_t[u] = jnp.transpose(jnp.broadcast_to(mid_bias[u : u + 1, :], (128, 128)))

    def project(u, s, values):
        normed = norm_rows(values, in_gain[u : u + 1, :], in_bias[u : u + 1, :]).astype(BF16)

        def part(first):
            return (
                lax.dot_general(
                    w_t[u, first : first + 128, :],
                    normed,
                    (((1,), (1,)), ((), ())),
                    preferred_element_type=F32,
                )
                + bias_t[u, first : first + 128, :]
            )

        tmp_r[pl.ds(s, 128, stride=8), :] = jax.nn.sigmoid(part(384)) * part(256)
        tmp_l[pl.ds(s, 128, stride=8), :] = jax.nn.sigmoid(part(128)) * part(0)
        gates[s] = jax.nn.sigmoid(
            jnp.dot(normed, proj_w[u, :, 512:640], preferred_element_type=F32)
            + proj_b[u : u + 1, 512:640]
        )

    def pack(u):
        def some(n, _):
            rows = pl.ds(n * 128, 128)
            send_r[u, pl.ds(n * 16, 16)] = tmp_r[rows, :].reshape(16, 8, 128).astype(BF16)
            send_l[u, pl.ds(n * 16, 16)] = tmp_l[rows, :].reshape(16, 8, 128).astype(BF16)
            return 0

        lax.fori_loop(0, 8, some, 0)

    def target(t):
        tz = lax.rem(z + lax.rem(t, 8), 8)
        tx = lax.rem(x + lax.rem(lax.div(t, 8), 4), 4)
        ty = lax.rem(y + lax.div(t, 32), 4)
        there = (ty * 4 + tx) * 8 + tz
        return there, ty * 2 + lax.div(tx, 2), tz * 4 + lax.rem(tx, 2) * 2

    def bytes_wait(buffer, sem):
        pltpu.make_async_copy(buffer, buffer, sem).wait()

    def send_right(u):
        slot = (core * 8 + row) * 16 + lax.div(col, 2)

        def one(t, _):
            there, trow, tcol = target(t)
            pltpu.make_async_remote_copy(
                send_r.at[u, there], recv_r.at[u, slot], sems_send.at[u, 0], sems_recv.at[u, 0],
                device_id=(trow, tcol + core), device_id_type=MESH,
            ).start()
            return 0

        lax.fori_loop(1, 128, one, 0)
        recv_r[u, slot] = send_r[u, chip]

    def send_left(u, half):
        if u == 0:
            slot = (core * 4 + lax.rem(row, 4)) * 16 + lax.div(col, 2)
        else:
            slot = (core * 8 + row) * 8 + lax.rem(lax.div(col, 2), 8)

        def one(t, _):
            there, trow, tcol = target(t)
            pltpu.make_async_remote_copy(
                send_l.at[u, there], recv_l.at[u, slot], sems_send.at[u, 1], sems_recv.at[u, 1],
                device_id=(trow, tcol + half), device_id_type=MESH,
            ).start()
            return 0

        lax.fori_loop(1, 128, one, 0)

        @pl.when(core == half)
        def _():
            recv_l[u, slot] = send_l[u, chip]

        @pl.when(core != half)
        def _():
            one(0, 0)

    def send_mixed(u):
        def one(t, _):
            tz = lax.rem(z + lax.rem(t, 8), 8)
            rest = lax.div(t, 8)
            tlow = lax.rem(low + lax.rem(rest, 4), 4)
            trow = lax.rem(row + lax.div(rest, 4), 4)
            tcol = tz * 4 + tlow
            pltpu.make_async_remote_copy(
                send_m.at[u, trow * 32 + tcol], recv_m.at[u, chip],
                sems_send.at[u, 2], sems_recv.at[u, 2],
                device_id=(core * 4 + trow, tcol), device_id_type=MESH,
            ).start()
            return 0

        lax.fori_loop(1, 128, one, 0)

        @pl.when(core == half_r)
        def _():
            recv_m[u, chip] = send_m[u, lax.rem(row, 4) * 32 + col]

        @pl.when(core != half_r)
        def _():
            one(0, 0)

    def wait_messages(buffer, sem, short):
        @pl.when(short)
        def _():
            bytes_wait(buffer.at[pl.ds(0, 127)], sem)

        @pl.when(jnp.logical_not(short))
        def _():
            bytes_wait(buffer, sem)

    def share_right(u):
        bytes_wait(recv_r.at[u, pl.ds(0, 127)], sems_recv.at[u, 0])
        mine = pl.ds(core * 128, 128)
        copy = pltpu.make_async_remote_copy(
            recv_r.at[u, mine], recv_r.at[u, mine], sems_send.at[u, 3], sems_recv.at[u, 3],
            device_id=(row, partner), device_id_type=MESH,
        )
        copy.start()
        return copy

    def woven(first, second):
        first, second = first.astype(F32), second.astype(F32)
        lane = lax.broadcasted_iota(jnp.int32, first.shape, 2)
        low_half = jnp.where(lane < 64, first, pltpu.roll(second, 64, 2))
        high_half = jnp.where(lane < 64, pltpu.roll(first, 64, 2), second)
        return jnp.concatenate([low_half, high_half], axis=1).astype(BF16)

    def arrange_right(u):
        for par in range(2):
            for p in range(4):
                base = (par * 8 + 2 * p) * 16
                a_r[:, par, :, p * 128 : (p + 1) * 128] = woven(
                    recv_r[u, base : base + 16], recv_r[u, base + 16 : base + 32]
                )

    def arrange_left(u):
        for par in range(2):
            if u == 0:
                for p in range(2):
                    base = (par * 4 + 2 * p) * 16
                    a_l0[:, par, :, p * 128 : (p + 1) * 128] = woven(
                        recv_l[u, base : base + 16], recv_l[u, base + 16 : base + 32]
                    )
            else:
                for p in range(4):
                    base = (par * 8 + 2 * p) * 8
                    a_l1[:, par, :, p * 128 : (p + 1) * 128] = woven(
                        recv_l[u, base : base + 8], recv_l[u, base + 8 : base + 16]
                    )

    def contract(u):
        right = a_r[...].reshape(512, 512)
        if u == 0:
            left = a_l0[...].reshape(512, 256)
            mixed[...] = lax.dot_general(
                right, left, (((0,), (0,)), ((), ())), preferred_element_type=F32
            )
        else:
            left = a_l1[...].reshape(256, 512)
            mixed[...] = lax.dot_general(
                right, left, (((1,), (1,)), ((), ())), preferred_element_type=F32
            )

    def pack_mixed(u):
        for p in range(2):
            both = mixed[:, p * 128 : (p + 1) * 128].reshape(32, 2, 8, 128)
            low_rows, high_rows = both[:, 0], both[:, 1]
            lane = lax.broadcasted_iota(jnp.int32, low_rows.shape, 2)
            send_m[u, 64 * p : 64 * p + 32] = jnp.where(
                lane < 64, low_rows, pltpu.roll(high_rows, 64, 2)
            ).astype(BF16)
            send_m[u, 64 * p + 32 : 64 * p + 64] = jnp.where(
                lane < 64, pltpu.roll(low_rows, 64, 2), high_rows
            ).astype(BF16)

    def normalise_mixed(u):
        def total(n, acc):
            return acc + jnp.sum(recv_m[u, pl.ds(n * 16, 16)].astype(F32), axis=0)

        mean = lax.fori_loop(0, 8, total, jnp.zeros((8, 128), F32)) * (1.0 / 128)

        def spread(n, acc):
            centred = recv_m[u, pl.ds(n * 16, 16)].astype(F32) - mean[None]
            return acc + jnp.sum(centred * centred, axis=0)

        variance = lax.fori_loop(0, 8, spread, jnp.zeros((8, 128), F32)) * (1.0 / 128)
        scale = lax.rsqrt(variance + EPS)

        def put(n, _):
            centred = recv_m[u, pl.ds(n * 16, 16)].astype(F32) - mean[None]
            tmp_l[pl.ds(n * 128, 128), :] = (centred * scale[None]).reshape(128, 128)
            return 0

        lax.fori_loop(0, 8, put, 0)

    def finish(u, s):
        middle = (tmp_l[pl.ds(s, 128, stride=8), :] * mgain_t[u] + mbias_t[u]).astype(BF16)
        outcome = (
            lax.dot_general(
                middle, out_w[u], (((0,), (0,)), ((), ())), preferred_element_type=F32
            )
            + out_b[u : u + 1, :]
        )
        return state[s] + gates[s] * outcome

    def exchange(u, half, cover):
        pack(u)
        send_right(u)
        send_left(u, half)
        cover()
        shared = share_right(u)
        wait_messages(recv_l.at[u], sems_recv.at[u, 1], core == half)
        arrange_left(u)
        shared.wait_recv()
        arrange_right(u)
        contract(u)
        pack_mixed(u)
        send_mixed(u)
        wait_messages(recv_m.at[u], sems_recv.at[u, 2], core == half_r)
        normalise_mixed(u)
        return shared

    prepare(0)

    def first(s, _):
        values = jnp.concatenate(
            [pair_ref[pl.ds(s, 64, stride=16), :], pair_ref[pl.ds(s + 8, 64, stride=16), :]], axis=0
        )
        state[s] = values
        project(0, s, values)
        return 0

    lax.fori_loop(0, 8, first, 0)

    pl.semaphore_wait(barrier, 38)

    def greet_again(t, _):
        pl.semaphore_signal(
            sem_enter, inc=1, device_id=(lax.rem(row + t, 8), col), device_id_type=MESH
        )
        return 0

    lax.fori_loop(1, 8, greet_again, 0)
    pl.semaphore_wait(sem_enter, 7)

    shared0 = exchange(0, half_r, lambda: prepare(1))

    def middle_step(s, _):
        values = finish(0, s)
        state[s] = values
        project(1, s, values)
        return 0

    lax.fori_loop(0, 8, middle_step, 0)

    shared1 = exchange(1, half_z, lambda: None)

    def last(s, _):
        values = finish(1, s)
        out_ref[pl.ds(s, 64, stride=16), :] = values[0:64]
        out_ref[pl.ds(s + 8, 64, stride=16), :] = values[64:128]
        return 0

    lax.fori_loop(0, 8, last, 0)

    for u, shared, half in ((0, shared0, half_r), (1, shared1, half_z)):
        shared.wait_send()
        bytes_wait(send_r.at[u, pl.ds(0, 127)], sems_send.at[u, 0])
        wait_messages(send_l.at[u], sems_send.at[u, 1], core == half)
        wait_messages(send_m.at[u], sems_send.at[u, 2], core == half_r)


def body(pair, in_gain, in_bias, proj_weight, proj_bias, mid_gain, mid_bias, out_weight, out_bias):
    vmem = pl.BlockSpec(memory_space=pltpu.VMEM)
    out = pl.pallas_call(
        kernel,
        out_shape=jax.ShapeDtypeStruct((1024, 128), F32),
        in_specs=[vmem] * 9,
        out_specs=vmem,
        scratch_shapes=[
            pltpu.VMEM((2, 512, 128), BF16),
            pltpu.VMEM((2, 512, 128), F32),
            pltpu.VMEM((2, 128, 128), F32),
            pltpu.VMEM((2, 128, 128), F32),
            pltpu.VMEM((8, 128, 128), F32),
            pltpu.VMEM((8, 128, 128), F32),
            pltpu.VMEM((1024, 128), F32),
            pltpu.VMEM((1024, 128), F32),
            pltpu.VMEM((2, 128, 8, 128), BF16),
            pltpu.VMEM((2, 128, 8, 128), BF16),
            pltpu.VMEM((2, 128, 8, 128), BF16),
            pltpu.VMEM((2, 128, 8, 128), BF16),
            pltpu.VMEM((2, 256, 8, 128), BF16),
            pltpu.VMEM((2, 128, 8, 128), BF16),
            pltpu.VMEM((16, 2, 16, 256), BF16),
            pltpu.VMEM((8, 2, 16, 512), BF16),
            pltpu.VMEM((16, 2, 16, 512), BF16),
            pltpu.VMEM((512, 256), F32),
            pltpu.SemaphoreType.DMA((2, 4)),
            pltpu.SemaphoreType.DMA((2, 4)),
            pltpu.SemaphoreType.REGULAR,
        ],
        compiler_params=pltpu.CompilerParams(
            collective_id=0, has_side_effects=True, vmem_limit_bytes=32 * 1024 * 1024
        ),
    )(
        pair.reshape(1024, 128), in_gain, in_bias, proj_weight, proj_bias,
        mid_gain, mid_bias, out_weight, out_bias,
    )
    return out.reshape(64, 16, 128)


def solution(mesh):
    placed = (P("row", "col", None), P(), P(), P(), P(), P(), P(), P(), P())
    return jax.shard_map(
        body, mesh=mesh, in_specs=placed, out_specs=P("row", "col", None), check_vma=False
    )
```

```python
import functools

import jax
import jax.numpy as jnp
from jax import lax
from jax.experimental import pallas as pl
from jax.experimental.pallas import tpu as pltpu
from jax.sharding import PartitionSpec as P

MESH = pl.DeviceIdType.MESH
F32 = jnp.float32
BF16 = jnp.bfloat16
EPS = 1e-05
FAR, SPLIT, CORE_FIRST = True, True, True


def norm_rows(values, gain, offset):
    mean = jnp.mean(values, -1, keepdims=True)
    centred = values - mean
    variance = jnp.mean(centred * centred, -1, keepdims=True)
    return centred * lax.rsqrt(variance + EPS) * gain + offset


def kernel(
    pair_in, in_gain_in, in_bias_in, proj_w_in, proj_b_in, mid_gain_in, mid_bias_in,
    out_w_in, out_b_in,
    out_ref,
    pair_ref, in_gain, in_bias, proj_w, proj_b, mid_gain, mid_bias, out_w, out_b, sems_in,
    w_t, bias_t, mgain_t, mbias_t,
    state, gates, tmp_l, tmp_r,
    send_l, send_r, send_m, recv_l, recv_r, recv_m,
    a_l0, a_l1, a_r, mixed,
    sems_send, sems_recv, sem_enter,
):
    row = lax.axis_index("row")
    col = lax.axis_index("col")
    y, xh = lax.div(row, 2), lax.rem(row, 2)
    z, low = lax.div(col, 4), lax.rem(col, 4)
    xl, core = lax.div(low, 2), lax.rem(low, 2)
    x = xh * 2 + xl
    chip = (y * 4 + x) * 8 + z
    partner = col + 1 - 2 * core
    half_r = lax.div(y, 2)
    half_z = lax.div(z, 4)

    barrier = pltpu.get_barrier_semaphore()

    def greet_row(t, _):
        pl.semaphore_signal(
            barrier, inc=1, device_id=(lax.rem(row + t, 8), col), device_id_type=MESH
        )
        return 0

    def greet_col(t, _):
        pl.semaphore_signal(
            barrier, inc=1, device_id=(row, lax.rem(col + t, 32)), device_id_type=MESH
        )
        return 0

    lax.fori_loop(1, 8, greet_row, 0)
    lax.fori_loop(1, 32, greet_col, 0)

    loads = [
        pltpu.make_async_copy(source, held, sems_in.at[n])
        for n, (source, held) in enumerate(
            (
                (proj_w_in, proj_w), (proj_b_in, proj_b), (mid_gain_in, mid_gain),
                (mid_bias_in, mid_bias), (in_gain_in, in_gain), (in_bias_in, in_bias),
                (pair_in, pair_ref), (out_w_in, out_w), (out_b_in, out_b),
            )
        )
    ]
    for load in loads:
        load.start()

    def prepare(u):
        w_t[u] = jnp.transpose(proj_w[u, :, 0:512].astype(F32)).astype(BF16)
        bias_t[u] = jnp.transpose(
            jnp.broadcast_to(proj_b[u : u + 1, 0:512], (128, 512))
        )
        mgain_t[u] = jnp.transpose(jnp.broadcast_to(mid_gain[u : u + 1, :], (128, 128)))
        mbias_t[u] = jnp.transpose(jnp.broadcast_to(mid_bias[u : u + 1, :], (128, 128)))

    def project(u, s, values):
        normed = norm_rows(values, in_gain[u : u + 1, :], in_bias[u : u + 1, :]).astype(BF16)

        def part(first):
            return (
                lax.dot_general(
                    w_t[u, first : first + 128, :],
                    normed,
                    (((1,), (1,)), ((), ())),
                    preferred_element_type=F32,
                )
                + bias_t[u, first : first + 128, :]
            )

        tmp_r[pl.ds(s, 128, stride=8), :] = jax.nn.sigmoid(part(384)) * part(256)
        tmp_l[pl.ds(s, 128, stride=8), :] = jax.nn.sigmoid(part(128)) * part(0)
        gates[s] = jax.nn.sigmoid(
            jnp.dot(normed, proj_w[u, :, 512:640], preferred_element_type=F32)
            + proj_b[u : u + 1, 512:640]
        )

    def pack(u):
        def some(n, _):
            rows = pl.ds(n * 128, 128)
            send_r[u, pl.ds(n * 16, 16)] = tmp_r[rows, :].reshape(16, 8, 128).astype(BF16)
            send_l[u, pl.ds(n * 16, 16)] = tmp_l[rows, :].reshape(16, 8, 128).astype(BF16)
            return 0

        lax.fori_loop(0, 8, some, 0)

    def place(tx, ty, tz):
        there = (ty * 4 + tx) * 8 + tz
        return there, ty * 2 + lax.div(tx, 2), tz * 4 + lax.rem(tx, 2) * 2

    def far(n, size):
        return lax.select(
            lax.rem(n, 2) == 1, size // 2 - lax.div(n + 1, 2), size // 2 + lax.div(n, 2)
        )

    def target(t):
        dz, dx, dy = lax.rem(t, 8), lax.rem(lax.div(t, 8), 4), lax.rem(lax.div(t, 32), 4)
        if FAR:
            dz, dx, dy = far(dz, 8), far(dx, 4), far(dy, 4)
        if not SPLIT:
            return place(lax.rem(x + dx, 4), lax.rem(y + dy, 4), lax.rem(z + dz, 8))
        part, rest = lax.div(t, 64), lax.rem(t, 64)
        dz, dx, dy = lax.rem(rest, 8), lax.rem(lax.div(rest, 8), 4), lax.div(rest, 32)
        if FAR:
            dz, dx, dy = far(dz, 8), far(dx, 4), 1 - dy
        tz, tx = lax.rem(z + dz, 8), lax.rem(x + dx, 4)
        ty = 2 * lax.rem(lax.div(y, 2) + dy, 2) + lax.rem(part + tx + tz, 2)
        return place(tx, ty, tz)

    def bytes_wait(buffer, sem):
        pltpu.make_async_copy(buffer, buffer, sem).wait()

    def exchange_sends(u, half):
        slot_r = (core * 8 + row) * 16 + lax.div(col, 2)
        if u == 0:
            slot_l = (core * 4 + lax.rem(row, 4)) * 16 + lax.div(col, 2)
        else:
            slot_l = (core * 8 + row) * 8 + lax.rem(lax.div(col, 2), 8)

        def right(t, _):
            there, trow, tcol = target(t)

            @pl.when(there != chip)
            def _():
                pltpu.make_async_remote_copy(
                    send_r.at[u, there], recv_r.at[u, slot_r],
                    sems_send.at[u, 0], sems_recv.at[u, 0],
                    device_id=(trow, tcol + core), device_id_type=MESH,
                ).start()

            return 0

        def left(t, _):
            there, trow, tcol = target(t)

            @pl.when(jnp.logical_or(there != chip, core != half))
            def _():
                pltpu.make_async_remote_copy(
                    send_l.at[u, there], recv_l.at[u, slot_l],
                    sems_send.at[u, 1], sems_recv.at[u, 1],
                    device_id=(trow, tcol + half), device_id_type=MESH,
                ).start()

            return 0

        if SPLIT:
            for part in range(2):
                lax.fori_loop(64 * part, 64 * part + 64, right, 0)
                lax.fori_loop(64 * part, 64 * part + 64, left, 0)
        else:
            lax.fori_loop(0, 128, right, 0)
            lax.fori_loop(0, 128, left, 0)
        recv_r[u, slot_r] = send_r[u, chip]

        @pl.when(core == half)
        def _():
            recv_l[u, slot_l] = send_l[u, chip]

    def send_mixed(u):
        def one(t, _):
            tz = lax.rem(t, 8)
            rest = lax.div(t, 8)
            if FAR:
                tz = far(tz, 8)
            tz = lax.rem(z + tz, 8)
            if CORE_FIRST and u == 0:
                tcore, rest = lax.div(rest, 8), lax.rem(rest, 8)
                if FAR:
                    rest = 7 - rest
                txl, rest = lax.rem(xl + rest, 2), lax.div(rest, 2)
                tlow = txl * 2 + tcore
            else:
                if FAR:
                    rest = 15 - rest
                tlow = lax.rem(low + lax.rem(rest, 4), 4)
                rest = lax.div(rest, 4)
            trow = lax.rem(row + rest, 4)
            tcol = tz * 4 + tlow

            @pl.when(jnp.logical_or(core * 4 + trow != row, tcol != col))
            def _():
                pltpu.make_async_remote_copy(
                    send_m.at[u, trow * 32 + tcol], recv_m.at[u, chip],
                    sems_send.at[u, 2], sems_recv.at[u, 2],
                    device_id=(core * 4 + trow, tcol), device_id_type=MESH,
                ).start()

            return 0

        lax.fori_loop(0, 128, one, 0)

        @pl.when(core == half_r)
        def _():
            recv_m[u, chip] = send_m[u, lax.rem(row, 4) * 32 + col]

    def wait_messages(buffer, sem, short):
        @pl.when(short)
        def _():
            bytes_wait(buffer.at[pl.ds(0, 127)], sem)

        @pl.when(jnp.logical_not(short))
        def _():
            bytes_wait(buffer, sem)

    def share_right(u):
        bytes_wait(recv_r.at[u, pl.ds(0, 127)], sems_recv.at[u, 0])
        mine = pl.ds(core * 128, 128)
        copy = pltpu.make_async_remote_copy(
            recv_r.at[u, mine], recv_r.at[u, mine], sems_send.at[u, 3], sems_recv.at[u, 3],
            device_id=(row, partner), device_id_type=MESH,
        )
        copy.start()
        return copy

    def woven(first, second):
        first, second = first.astype(F32), second.astype(F32)
        lane = lax.broadcasted_iota(jnp.int32, first.shape, 2)
        low_half = jnp.where(lane < 64, first, pltpu.roll(second, 64, 2))
        high_half = jnp.where(lane < 64, pltpu.roll(first, 64, 2), second)
        return jnp.concatenate([low_half, high_half], axis=1).astype(BF16)

    def arrange_right(u):
        for par in range(2):
            for p in range(4):
                base = (par * 8 + 2 * p) * 16
                a_r[:, par, :, p * 128 : (p + 1) * 128] = woven(
                    recv_r[u, base : base + 16], recv_r[u, base + 16 : base + 32]
                )

    def arrange_left(u):
        for par in range(2):
            if u == 0:
                for p in range(2):
                    base = (par * 4 + 2 * p) * 16
                    a_l0[:, par, :, p * 128 : (p + 1) * 128] = woven(
                        recv_l[u, base : base + 16], recv_l[u, base + 16 : base + 32]
                    )
            else:
                for p in range(4):
                    base = (par * 8 + 2 * p) * 8
                    a_l1[:, par, :, p * 128 : (p + 1) * 128] = woven(
                        recv_l[u, base : base + 8], recv_l[u, base + 8 : base + 16]
                    )

    def contract(u):
        right = a_r[...].reshape(512, 512)
        if u == 0:
            left = a_l0[...].reshape(512, 256)
            mixed[...] = lax.dot_general(
                right, left, (((0,), (0,)), ((), ())), preferred_element_type=F32
            )
        else:
            left = a_l1[...].reshape(256, 512)
            mixed[...] = lax.dot_general(
                right, left, (((1,), (1,)), ((), ())), preferred_element_type=F32
            )

    def pack_mixed(u):
        for p in range(2):
            both = mixed[:, p * 128 : (p + 1) * 128].reshape(32, 2, 8, 128)
            low_rows, high_rows = both[:, 0], both[:, 1]
            lane = lax.broadcasted_iota(jnp.int32, low_rows.shape, 2)
            send_m[u, 64 * p : 64 * p + 32] = jnp.where(
                lane < 64, low_rows, pltpu.roll(high_rows, 64, 2)
            ).astype(BF16)
            send_m[u, 64 * p + 32 : 64 * p + 64] = jnp.where(
                lane < 64, pltpu.roll(low_rows, 64, 2), high_rows
            ).astype(BF16)

    def normalise_mixed(u):
        def total(n, acc):
            return acc + jnp.sum(recv_m[u, pl.ds(n * 16, 16)].astype(F32), axis=0)

        mean = lax.fori_loop(0, 8, total, jnp.zeros((8, 128), F32)) * (1.0 / 128)

        def spread(n, acc):
            centred = recv_m[u, pl.ds(n * 16, 16)].astype(F32) - mean[None]
            return acc + jnp.sum(centred * centred, axis=0)

        variance = lax.fori_loop(0, 8, spread, jnp.zeros((8, 128), F32)) * (1.0 / 128)
        scale = lax.rsqrt(variance + EPS)

        def put(n, _):
            centred = recv_m[u, pl.ds(n * 16, 16)].astype(F32) - mean[None]
            tmp_l[pl.ds(n * 128, 128), :] = (centred * scale[None]).reshape(128, 128)
            return 0

        lax.fori_loop(0, 8, put, 0)

    def finish(u, s):
        middle = (tmp_l[pl.ds(s, 128, stride=8), :] * mgain_t[u] + mbias_t[u]).astype(BF16)
        outcome = (
            lax.dot_general(
                middle, out_w[u], (((0,), (0,)), ((), ())), preferred_element_type=F32
            )
            + out_b[u : u + 1, :]
        )
        return state[s] + gates[s] * outcome

    def exchange(u, half, cover):
        pack(u)
        exchange_sends(u, half)
        cover()
        shared = share_right(u)
        shared.wait_recv()
        arrange_right(u)
        wait_messages(recv_l.at[u], sems_recv.at[u, 1], core == half)
        arrange_left(u)
        contract(u)
        pack_mixed(u)
        send_mixed(u)
        wait_messages(recv_m.at[u], sems_recv.at[u, 2], core == half_r)
        normalise_mixed(u)
        return shared

    for load in loads:
        load.wait()
    prepare(0)

    def first(s, _):
        values = jnp.concatenate(
            [pair_ref[pl.ds(s, 64, stride=16), :], pair_ref[pl.ds(s + 8, 64, stride=16), :]], axis=0
        )
        state[s] = values
        project(0, s, values)
        return 0

    lax.fori_loop(0, 8, first, 0)

    pl.semaphore_wait(barrier, 38)

    def greet_again(t, _):
        pl.semaphore_signal(
            sem_enter, inc=1, device_id=(lax.rem(row + t, 8), col), device_id_type=MESH
        )
        return 0

    lax.fori_loop(1, 8, greet_again, 0)
    pl.semaphore_wait(sem_enter, 7)

    shared0 = exchange(0, half_r, lambda: prepare(1))

    def middle_step(s, _):
        values = finish(0, s)
        state[s] = values
        project(1, s, values)
        return 0

    lax.fori_loop(0, 8, middle_step, 0)

    shared1 = exchange(1, half_z, lambda: None)

    def last(s, _):
        values = finish(1, s)
        out_ref[pl.ds(s, 64, stride=16), :] = values[0:64]
        out_ref[pl.ds(s + 8, 64, stride=16), :] = values[64:128]
        return 0

    lax.fori_loop(0, 8, last, 0)

    for u, shared, half in ((0, shared0, half_r), (1, shared1, half_z)):
        shared.wait_send()
        bytes_wait(send_r.at[u, pl.ds(0, 127)], sems_send.at[u, 0])
        wait_messages(send_l.at[u], sems_send.at[u, 1], core == half)
        wait_messages(send_m.at[u], sems_send.at[u, 2], core == half_r)


def body(pair, in_gain, in_bias, proj_weight, proj_bias, mid_gain, mid_bias, out_weight, out_bias):
    vmem = pl.BlockSpec(memory_space=pltpu.VMEM)
    out = pl.pallas_call(
        kernel,
        out_shape=jax.ShapeDtypeStruct((1024, 128), F32),
        in_specs=[pl.BlockSpec(memory_space=pltpu.HBM)] * 9,
        out_specs=vmem,
        scratch_shapes=[
            pltpu.VMEM((1024, 128), F32),
            pltpu.VMEM((2, 128), F32),
            pltpu.VMEM((2, 128), F32),
            pltpu.VMEM((2, 128, 640), BF16),
            pltpu.VMEM((2, 640), F32),
            pltpu.VMEM((2, 128), F32),
            pltpu.VMEM((2, 128), F32),
            pltpu.VMEM((2, 128, 128), BF16),
            pltpu.VMEM((2, 128), F32),
            pltpu.SemaphoreType.DMA((9,)),
            pltpu.VMEM((2, 512, 128), BF16),
            pltpu.VMEM((2, 512, 128), F32),
            pltpu.VMEM((2, 128, 128), F32),
            pltpu.VMEM((2, 128, 128), F32),
            pltpu.VMEM((8, 128, 128), F32),
            pltpu.VMEM((8, 128, 128), F32),
            pltpu.VMEM((1024, 128), F32),
            pltpu.VMEM((1024, 128), F32),
            pltpu.VMEM((2, 128, 8, 128), BF16),
            pltpu.VMEM((2, 128, 8, 128), BF16),
            pltpu.VMEM((2, 128, 8, 128), BF16),
            pltpu.VMEM((2, 128, 8, 128), BF16),
            pltpu.VMEM((2, 256, 8, 128), BF16),
            pltpu.VMEM((2, 128, 8, 128), BF16),
            pltpu.VMEM((16, 2, 16, 256), BF16),
            pltpu.VMEM((8, 2, 16, 512), BF16),
            pltpu.VMEM((16, 2, 16, 512), BF16),
            pltpu.VMEM((512, 256), F32),
            pltpu.SemaphoreType.DMA((2, 4)),
            pltpu.SemaphoreType.DMA((2, 4)),
            pltpu.SemaphoreType.REGULAR,
        ],
        compiler_params=pltpu.CompilerParams(
            collective_id=0, has_side_effects=True
        ),
    )(
        pair.reshape(1024, 128), in_gain, in_bias, proj_weight, proj_bias,
        mid_gain, mid_bias, out_weight, out_bias,
    )
    return out.reshape(64, 16, 128)


def solution(mesh):
    placed = (P("row", "col", None), P(), P(), P(), P(), P(), P(), P(), P())
    return jax.shard_map(
        body, mesh=mesh, in_specs=placed, out_specs=P("row", "col", None), check_vma=False
    )
```

```python
import functools

import jax
import jax.numpy as jnp
from jax import lax
from jax.experimental import pallas as pl
from jax.experimental.pallas import tpu as pltpu
from jax.sharding import PartitionSpec as P

MESH = pl.DeviceIdType.MESH
F32 = jnp.float32
BF16 = jnp.bfloat16
EPS = 1e-05
FAR, SPLIT, CORE_FIRST = True, True, True


def twice(column):
    return jnp.concatenate([column, column], axis=1)


def norm_channels(values, gain, offset):
    mean = jnp.mean(values, 0, keepdims=True)
    centred = values - mean
    variance = jnp.mean(centred * centred, 0, keepdims=True)
    return (centred * lax.rsqrt(variance + EPS) * twice(gain) + twice(offset)).astype(BF16)


def kernel(
    pair_in, in_gain_in, in_bias_in, proj_w_in, proj_b_in, mid_gain_in, mid_bias_in,
    out_w_in, out_b_in,
    out_ref,
    pair_ref, in_gain, in_bias, proj_w, proj_b, mid_gain, mid_bias, out_w, out_b, sems_in,
    w_t, ow_t, bias_t, igain_t, ibias_t, mgain_t, mbias_t, obias_t,
    state, gates, tmp_l, tmp_r, tmp_m,
    send_l, send_r, send_m, recv_l, recv_r, recv_m,
    a_l0, a_l1, a_r, mixed,
    sems_send, sems_recv, sem_enter,
):
    row = lax.axis_index("row")
    col = lax.axis_index("col")
    y, xh = lax.div(row, 2), lax.rem(row, 2)
    z, low = lax.div(col, 4), lax.rem(col, 4)
    xl, core = lax.div(low, 2), lax.rem(low, 2)
    x = xh * 2 + xl
    chip = (y * 4 + x) * 8 + z
    partner = col + 1 - 2 * core
    half_r = lax.div(y, 2)
    half_z = lax.div(z, 4)

    barrier = pltpu.get_barrier_semaphore()

    def greet_row(t, _):
        pl.semaphore_signal(
            barrier, inc=1, device_id=(lax.rem(row + t, 8), col), device_id_type=MESH
        )
        return 0

    def greet_col(t, _):
        pl.semaphore_signal(
            barrier, inc=1, device_id=(row, lax.rem(col + t, 32)), device_id_type=MESH
        )
        return 0

    lax.fori_loop(1, 8, greet_row, 0)
    lax.fori_loop(1, 32, greet_col, 0)

    loads = [
        pltpu.make_async_copy(source, held, sems_in.at[n])
        for n, (source, held) in enumerate(
            (
                (proj_w_in, proj_w), (proj_b_in, proj_b), (mid_gain_in, mid_gain),
                (mid_bias_in, mid_bias), (in_gain_in, in_gain), (in_bias_in, in_bias),
                (pair_in, pair_ref), (out_w_in, out_w), (out_b_in, out_b),
            )
        )
    ]
    for load in loads:
        load.start()

    def column(held, u):
        return jnp.transpose(jnp.broadcast_to(held[u : u + 1, :], (128, held.shape[1])))

    def prepare_projection(u):
        w_t[u] = jnp.transpose(proj_w[u].astype(F32)).astype(BF16)
        igain_t[u] = column(in_gain, u)
        ibias_t[u] = column(in_bias, u)
        bias_t[u] = column(proj_b, u)

    def prepare_finish(u):
        ow_t[u] = jnp.transpose(out_w[u].astype(F32)).astype(BF16)
        mgain_t[u] = column(mid_gain, u)
        mbias_t[u] = column(mid_bias, u)
        obias_t[u] = column(out_b, u)

    def project(u, n, values):
        normed = norm_channels(values, igain_t[u], ibias_t[u])

        def part(first):
            return jnp.dot(
                w_t[u, first : first + 128, :], normed, preferred_element_type=F32
            ) + twice(bias_t[u, first : first + 128, :])

        right = jax.nn.sigmoid(part(384)) * part(256)
        left = jax.nn.sigmoid(part(128)) * part(0)
        for k in range(2):
            rows = pl.ds(2 * n + k, 128, stride=8)
            tmp_r[rows, :] = right[:, 128 * k : 128 * k + 128]
            tmp_l[rows, :] = left[:, 128 * k : 128 * k + 128]
        gates[n] = jax.nn.sigmoid(part(512))

    def pack(u):
        def some(n, _):
            rows = pl.ds(n * 128, 128)
            send_r[u, pl.ds(n * 16, 16)] = tmp_r[rows, :].reshape(16, 8, 128).astype(BF16)
            send_l[u, pl.ds(n * 16, 16)] = tmp_l[rows, :].reshape(16, 8, 128).astype(BF16)
            return 0

        lax.fori_loop(0, 8, some, 0)

    def place(tx, ty, tz):
        there = (ty * 4 + tx) * 8 + tz
        return there, ty * 2 + lax.div(tx, 2), tz * 4 + lax.rem(tx, 2) * 2

    def far(n, size):
        return lax.select(
            lax.rem(n, 2) == 1, size // 2 - lax.div(n + 1, 2), size // 2 + lax.div(n, 2)
        )

    def target(t):
        dz, dx, dy = lax.rem(t, 8), lax.rem(lax.div(t, 8), 4), lax.rem(lax.div(t, 32), 4)
        if FAR:
            dz, dx, dy = far(dz, 8), far(dx, 4), far(dy, 4)
        if not SPLIT:
            return place(lax.rem(x + dx, 4), lax.rem(y + dy, 4), lax.rem(z + dz, 8))
        part, rest = lax.div(t, 64), lax.rem(t, 64)
        dz, dx, dy = lax.rem(rest, 8), lax.rem(lax.div(rest, 8), 4), lax.div(rest, 32)
        if FAR:
            dz, dx, dy = far(dz, 8), far(dx, 4), 1 - dy
        tz, tx = lax.rem(z + dz, 8), lax.rem(x + dx, 4)
        ty = 2 * lax.rem(lax.div(y, 2) + dy, 2) + lax.rem(part + tx + tz, 2)
        return place(tx, ty, tz)

    def bytes_wait(buffer, sem):
        pltpu.make_async_copy(buffer, buffer, sem).wait()

    def exchange_sends(u, half):
        slot_r = (core * 8 + row) * 16 + lax.div(col, 2)
        if u == 0:
            slot_l = (core * 4 + lax.rem(row, 4)) * 16 + lax.div(col, 2)
        else:
            slot_l = (core * 8 + row) * 8 + lax.rem(lax.div(col, 2), 8)

        def right(t, _):
            there, trow, tcol = target(t)

            @pl.when(there != chip)
            def _():
                pltpu.make_async_remote_copy(
                    send_r.at[u, there], recv_r.at[u, slot_r],
                    sems_send.at[u, 0], sems_recv.at[u, 0],
                    device_id=(trow, tcol + core), device_id_type=MESH,
                ).start()

            return 0

        def left(t, _):
            there, trow, tcol = target(t)

            @pl.when(jnp.logical_or(there != chip, core != half))
            def _():
                pltpu.make_async_remote_copy(
                    send_l.at[u, there], recv_l.at[u, slot_l],
                    sems_send.at[u, 1], sems_recv.at[u, 1],
                    device_id=(trow, tcol + half), device_id_type=MESH,
                ).start()

            return 0

        if SPLIT:
            for part in range(2):
                lax.fori_loop(64 * part, 64 * part + 64, right, 0)
                lax.fori_loop(64 * part, 64 * part + 64, left, 0)
        else:
            lax.fori_loop(0, 128, right, 0)
            lax.fori_loop(0, 128, left, 0)
        recv_r[u, slot_r] = send_r[u, chip]

        @pl.when(core == half)
        def _():
            recv_l[u, slot_l] = send_l[u, chip]

    def send_mixed(u):
        def one(t, _):
            tz = lax.rem(t, 8)
            rest = lax.div(t, 8)
            if FAR:
                tz = far(tz, 8)
            tz = lax.rem(z + tz, 8)
            if CORE_FIRST and u == 0:
                tcore, rest = lax.div(rest, 8), lax.rem(rest, 8)
                if FAR:
                    rest = 7 - rest
                txl, rest = lax.rem(xl + rest, 2), lax.div(rest, 2)
                tlow = txl * 2 + tcore
            else:
                if FAR:
                    rest = 15 - rest
                tlow = lax.rem(low + lax.rem(rest, 4), 4)
                rest = lax.div(rest, 4)
            trow = lax.rem(row + rest, 4)
            tcol = tz * 4 + tlow

            @pl.when(jnp.logical_or(core * 4 + trow != row, tcol != col))
            def _():
                pltpu.make_async_remote_copy(
                    send_m.at[u, trow * 32 + tcol], recv_m.at[u, chip],
                    sems_send.at[u, 2], sems_recv.at[u, 2],
                    device_id=(core * 4 + trow, tcol), device_id_type=MESH,
                ).start()

            return 0

        lax.fori_loop(0, 128, one, 0)

        @pl.when(core == half_r)
        def _():
            recv_m[u, chip] = send_m[u, lax.rem(row, 4) * 32 + col]

    def wait_messages(buffer, sem, short):
        @pl.when(short)
        def _():
            bytes_wait(buffer.at[pl.ds(0, 127)], sem)

        @pl.when(jnp.logical_not(short))
        def _():
            bytes_wait(buffer, sem)

    def share_right(u):
        bytes_wait(recv_r.at[u, pl.ds(0, 127)], sems_recv.at[u, 0])
        mine = pl.ds(core * 128, 128)
        copy = pltpu.make_async_remote_copy(
            recv_r.at[u, mine], recv_r.at[u, mine], sems_send.at[u, 3], sems_recv.at[u, 3],
            device_id=(row, partner), device_id_type=MESH,
        )
        copy.start()
        return copy

    def woven(first, second):
        first, second = first.astype(F32), second.astype(F32)
        lane = lax.broadcasted_iota(jnp.int32, first.shape, 2)
        low_half = jnp.where(lane < 64, first, pltpu.roll(second, 64, 2))
        high_half = jnp.where(lane < 64, pltpu.roll(first, 64, 2), second)
        return jnp.concatenate([low_half, high_half], axis=1).astype(BF16)

    def arrange_right(u):
        for par in range(2):
            for p in range(4):
                base = (par * 8 + 2 * p) * 16
                a_r[:, par, :, p * 128 : (p + 1) * 128] = woven(
                    recv_r[u, base : base + 16], recv_r[u, base + 16 : base + 32]
                )

    def arrange_left(u):
        for par in range(2):
            if u == 0:
                for p in range(2):
                    base = (par * 4 + 2 * p) * 16
                    a_l0[:, par, :, p * 128 : (p + 1) * 128] = woven(
                        recv_l[u, base : base + 16], recv_l[u, base + 16 : base + 32]
                    )
            else:
                for p in range(4):
                    base = (par * 8 + 2 * p) * 8
                    a_l1[:, par, :, p * 128 : (p + 1) * 128] = woven(
                        recv_l[u, base : base + 8], recv_l[u, base + 8 : base + 16]
                    )

    def contract(u):
        right = a_r[...].reshape(512, 512)
        if u == 0:
            left = a_l0[...].reshape(512, 256)
            mixed[...] = lax.dot_general(
                right, left, (((0,), (0,)), ((), ())), preferred_element_type=F32
            )
        else:
            left = a_l1[...].reshape(256, 512)
            mixed[...] = lax.dot_general(
                right, left, (((1,), (1,)), ((), ())), preferred_element_type=F32
            )

    def pack_mixed(u):
        for p in range(2):
            both = mixed[:, p * 128 : (p + 1) * 128].reshape(32, 2, 8, 128)
            low_rows, high_rows = both[:, 0], both[:, 1]
            lane = lax.broadcasted_iota(jnp.int32, low_rows.shape, 2)
            send_m[u, 64 * p : 64 * p + 32] = jnp.where(
                lane < 64, low_rows, pltpu.roll(high_rows, 64, 2)
            ).astype(BF16)
            send_m[u, 64 * p + 32 : 64 * p + 64] = jnp.where(
                lane < 64, pltpu.roll(low_rows, 64, 2), high_rows
            ).astype(BF16)

    def widen_mixed(u):
        def put(n, _):
            tmp_m[pl.ds(n * 128, 128), :] = (
                recv_m[u, pl.ds(n * 16, 16)].astype(F32).reshape(128, 128)
            )
            return 0

        lax.fori_loop(0, 8, put, 0, unroll=True)

    def finish(u, n):
        values = jnp.concatenate(
            [tmp_m[pl.ds(2 * n + k, 128, stride=8), :] for k in range(2)], axis=1
        )
        middle = norm_channels(values, mgain_t[u], mbias_t[u])
        outcome = jnp.dot(ow_t[u], middle, preferred_element_type=F32) + twice(obias_t[u])
        return state[n] + gates[n] * outcome

    def exchange(u, half, cover):
        pack(u)
        exchange_sends(u, half)
        cover()
        shared = share_right(u)
        shared.wait_recv()
        arrange_right(u)
        wait_messages(recv_l.at[u], sems_recv.at[u, 1], core == half)
        arrange_left(u)
        contract(u)
        pack_mixed(u)
        send_mixed(u)
        wait_messages(recv_m.at[u], sems_recv.at[u, 2], core == half_r)
        widen_mixed(u)
        return shared

    for load in loads:
        load.wait()
    prepare_projection(0)

    for n in range(4):
        blocks = [
            jnp.concatenate(
                [pair_ref[pl.ds(s, 64, stride=16), :], pair_ref[pl.ds(s + 8, 64, stride=16), :]],
                axis=0,
            )
            for s in (2 * n, 2 * n + 1)
        ]
        values = jnp.concatenate([jnp.transpose(block) for block in blocks], axis=1)
        state[n] = values
        project(0, n, values)

    pl.semaphore_wait(barrier, 38)

    def greet_again(t, _):
        pl.semaphore_signal(
            sem_enter, inc=1, device_id=(lax.rem(row + t, 8), col), device_id_type=MESH
        )
        return 0

    lax.fori_loop(1, 8, greet_again, 0)
    pl.semaphore_wait(sem_enter, 7)

    def cover():
        prepare_finish(0)
        prepare_projection(1)
        prepare_finish(1)

    shared0 = exchange(0, half_r, cover)

    for n in range(4):
        values = finish(0, n)
        state[n] = values
        project(1, n, values)

    shared1 = exchange(1, half_z, lambda: None)

    for n in range(4):
        values = finish(1, n)
        for k in range(2):
            s = 2 * n + k
            block = jnp.transpose(values[:, 128 * k : 128 * k + 128])
            out_ref[pl.ds(s, 64, stride=16), :] = block[0:64]
            out_ref[pl.ds(s + 8, 64, stride=16), :] = block[64:128]

    for u, shared, half in ((0, shared0, half_r), (1, shared1, half_z)):
        shared.wait_send()
        bytes_wait(send_r.at[u, pl.ds(0, 127)], sems_send.at[u, 0])
        wait_messages(send_l.at[u], sems_send.at[u, 1], core == half)
        wait_messages(send_m.at[u], sems_send.at[u, 2], core == half_r)


def body(pair, in_gain, in_bias, proj_weight, proj_bias, mid_gain, mid_bias, out_weight, out_bias):
    vmem = pl.BlockSpec(memory_space=pltpu.VMEM)
    out = pl.pallas_call(
        kernel,
        out_shape=jax.ShapeDtypeStruct((1024, 128), F32),
        in_specs=[pl.BlockSpec(memory_space=pltpu.HBM)] * 9,
        out_specs=vmem,
        scratch_shapes=[
            pltpu.VMEM((1024, 128), F32),
            pltpu.VMEM((2, 128), F32),
            pltpu.VMEM((2, 128), F32),
            pltpu.VMEM((2, 128, 640), BF16),
            pltpu.VMEM((2, 640), F32),
            pltpu.VMEM((2, 128), F32),
            pltpu.VMEM((2, 128), F32),
            pltpu.VMEM((2, 128, 128), BF16),
            pltpu.VMEM((2, 128), F32),
            pltpu.SemaphoreType.DMA((9,)),
            pltpu.VMEM((2, 640, 128), BF16),
            pltpu.VMEM((2, 128, 128), BF16),
            pltpu.VMEM((2, 640, 128), F32),
            pltpu.VMEM((2, 128, 128), F32),
            pltpu.VMEM((2, 128, 128), F32),
            pltpu.VMEM((2, 128, 128), F32),
            pltpu.VMEM((2, 128, 128), F32),
            pltpu.VMEM((2, 128, 128), F32),
            pltpu.VMEM((4, 128, 256), F32),
            pltpu.VMEM((4, 128, 256), F32),
            pltpu.VMEM((1024, 128), F32),
            pltpu.VMEM((1024, 128), F32),
            pltpu.VMEM((1024, 128), F32),
            pltpu.VMEM((2, 128, 8, 128), BF16),
            pltpu.VMEM((2, 128, 8, 128), BF16),
            pltpu.VMEM((2, 128, 8, 128), BF16),
            pltpu.VMEM((2, 128, 8, 128), BF16),
            pltpu.VMEM((2, 256, 8, 128), BF16),
            pltpu.VMEM((2, 128, 8, 128), BF16),
            pltpu.VMEM((16, 2, 16, 256), BF16),
            pltpu.VMEM((8, 2, 16, 512), BF16),
            pltpu.VMEM((16, 2, 16, 512), BF16),
            pltpu.VMEM((512, 256), F32),
            pltpu.SemaphoreType.DMA((2, 4)),
            pltpu.SemaphoreType.DMA((2, 4)),
            pltpu.SemaphoreType.REGULAR,
        ],
        compiler_params=pltpu.CompilerParams(
            collective_id=0, has_side_effects=True
        ),
    )(
        pair.reshape(1024, 128), in_gain, in_bias, proj_weight, proj_bias,
        mid_gain, mid_bias, out_weight, out_bias,
    )
    return out.reshape(64, 16, 128)


def solution(mesh):
    placed = (P("row", "col", None), P(), P(), P(), P(), P(), P(), P(), P())
    return jax.shard_map(
        body, mesh=mesh, in_specs=placed, out_specs=P("row", "col", None), check_vma=False
    )
```

```python
import functools

import jax
import jax.numpy as jnp
from jax import lax
from jax.experimental import pallas as pl
from jax.experimental.pallas import tpu as pltpu
from jax.sharding import PartitionSpec as P

MESH = pl.DeviceIdType.MESH
F32 = jnp.float32
BF16 = jnp.bfloat16
EPS = 1e-05
UNROLL = 8


def twice(column):
    return jnp.concatenate([column, column], axis=1)


def norm_channels(values, gain, offset):
    mean = jnp.mean(values, 0, keepdims=True)
    centred = values - mean
    variance = jnp.mean(centred * centred, 0, keepdims=True)
    return (centred * lax.rsqrt(variance + EPS) * twice(gain) + twice(offset)).astype(BF16)


def kernel(
    pair_in, in_gain_in, in_bias_in, proj_w_in, proj_b_in, mid_gain_in, mid_bias_in,
    out_w_in, out_b_in,
    out_ref,
    pair_ref, in_gain, in_bias, proj_w, proj_b, mid_gain, mid_bias, out_w, out_b, sems_in,
    w_t, ow_t, bias_t, igain_t, ibias_t, mgain_t, mbias_t, obias_t,
    state, gates, tmp_l, tmp_r, tmp_m,
    send_l, send_r, send_m, recv_l, recv_r, recv_m,
    a_l0, a_l1, a_r, a_rt, normed,
    sems_send, sems_recv, sem_enter,
):
    row = lax.axis_index("row")
    col = lax.axis_index("col")
    y, xh = lax.div(row, 2), lax.rem(row, 2)
    z, low = lax.div(col, 4), lax.rem(col, 4)
    xl, core = lax.div(low, 2), lax.rem(low, 2)
    x = xh * 2 + xl
    chip = (y * 4 + x) * 8 + z
    partner = col + 1 - 2 * core
    half_r = lax.div(y, 2)
    half_z = lax.div(z, 4)

    barrier = pltpu.get_barrier_semaphore()

    def greet_row(t, _):
        pl.semaphore_signal(
            barrier, inc=1, device_id=(lax.rem(row + t, 8), col), device_id_type=MESH
        )
        return 0

    def greet_col(t, _):
        pl.semaphore_signal(
            barrier, inc=1, device_id=(row, lax.rem(col + t, 32)), device_id_type=MESH
        )
        return 0

    lax.fori_loop(1, 8, greet_row, 0)
    lax.fori_loop(1, 32, greet_col, 0)

    loads = [
        pltpu.make_async_copy(source, held, sems_in.at[n])
        for n, (source, held) in enumerate(
            (
                (proj_w_in, proj_w), (proj_b_in, proj_b), (mid_gain_in, mid_gain),
                (mid_bias_in, mid_bias), (in_gain_in, in_gain), (in_bias_in, in_bias),
                (pair_in, pair_ref), (out_w_in, out_w), (out_b_in, out_b),
            )
        )
    ]
    for load in loads:
        load.start()

    def column(held, u):
        return jnp.transpose(jnp.broadcast_to(held[u : u + 1, :], (128, held.shape[1])))

    def prepare_projection(u):
        w_t[u] = jnp.transpose(proj_w[u].astype(F32)).astype(BF16)
        igain_t[u] = column(in_gain, u)
        ibias_t[u] = column(in_bias, u)
        bias_t[u] = column(proj_b, u)

    def prepare_finish(u):
        ow_t[u] = jnp.transpose(out_w[u].astype(F32)).astype(BF16)
        mgain_t[u] = column(mid_gain, u)
        mbias_t[u] = column(mid_bias, u)
        obias_t[u] = column(out_b, u)

    def normalise(u, n, values):
        normed[n] = norm_channels(values, igain_t[u], ibias_t[u])

    def part(u, n, first):
        return jnp.dot(
            w_t[u, first : first + 128, :], normed[n], preferred_element_type=F32
        ) + twice(bias_t[u, first : first + 128, :])

    def project(u, first, held, packed):
        for n in range(4):
            values = jax.nn.sigmoid(part(u, n, first + 128)) * part(u, n, first)
            for k in range(2):
                held[pl.ds(2 * n + k, 128, stride=8), :] = values[:, 128 * k : 128 * k + 128]
        for n in range(8):
            packed[u, 16 * n : 16 * n + 16] = (
                held[128 * n : 128 * n + 128, :].reshape(16, 8, 128).astype(BF16)
            )

    def open_gates(u):
        for n in range(4):
            gates[n] = jax.nn.sigmoid(part(u, n, 512))

    def place(tx, ty, tz):
        there = (ty * 4 + tx) * 8 + tz
        return there, ty * 2 + lax.div(tx, 2), tz * 4 + lax.rem(tx, 2) * 2

    def far(n, size):
        return lax.select(
            lax.rem(n, 2) == 1, size // 2 - lax.div(n + 1, 2), size // 2 + lax.div(n, 2)
        )

    def target(t):
        part, rest = lax.div(t, 64), lax.rem(t, 64)
        tz = lax.rem(z + far(lax.rem(rest, 8), 8), 8)
        tx = lax.rem(x + far(lax.rem(lax.div(rest, 8), 4), 4), 4)
        ty = 2 * lax.rem(lax.div(y, 2) + 1 - lax.div(rest, 32), 2) + lax.rem(part + tx + tz, 2)
        return place(tx, ty, tz)

    def bytes_wait(buffer, sem):
        pltpu.make_async_copy(buffer, buffer, sem).wait()

    def send_right(u, part):
        slot = (core * 8 + row) * 16 + lax.div(col, 2)

        def one(t, _):
            there, trow, tcol = target(t)

            @pl.when(there != chip)
            def _():
                pltpu.make_async_remote_copy(
                    send_r.at[u, there], recv_r.at[u, slot],
                    sems_send.at[u, 0], sems_recv.at[u, 0],
                    device_id=(trow, tcol + core), device_id_type=MESH,
                ).start()

            return 0

        lax.fori_loop(64 * part, 64 * part + 64, one, 0, unroll=UNROLL)
        if part == 1:
            recv_r[u, slot] = send_r[u, chip]

    def send_left(u, half, part):
        if u == 0:
            slot = (core * 4 + lax.rem(row, 4)) * 16 + lax.div(col, 2)
        else:
            slot = (core * 8 + row) * 8 + lax.rem(lax.div(col, 2), 8)

        def one(t, _):
            there, trow, tcol = target(t)

            @pl.when(jnp.logical_or(there != chip, core != half))
            def _():
                pltpu.make_async_remote_copy(
                    send_l.at[u, there], recv_l.at[u, slot],
                    sems_send.at[u, 1], sems_recv.at[u, 1],
                    device_id=(trow, tcol + half), device_id_type=MESH,
                ).start()

            return 0

        lax.fori_loop(64 * part, 64 * part + 64, one, 0, unroll=UNROLL)
        if part == 1:

            @pl.when(core == half)
            def _():
                recv_l[u, slot] = send_l[u, chip]

    def send_mixed(u):
        def one(t, _):
            if u == 0:
                tz = lax.rem(z + far(lax.rem(lax.div(t, 8), 8), 8), 8)
                rest = 7 - lax.rem(t, 8)
                tlow = lax.rem(xl + rest, 2) * 2 + lax.div(t, 64)
                trow = lax.rem(row + lax.div(rest, 2), 4)
            else:
                tz = lax.rem(z + far(lax.div(t, 16), 8), 8)
                rest = 15 - lax.rem(t, 16)
                tlow = lax.rem(low + lax.rem(rest, 4), 4)
                trow = lax.rem(row + lax.div(rest, 4), 4)
            tcol = tz * 4 + tlow

            @pl.when(jnp.logical_or(core * 4 + trow != row, tcol != col))
            def _():
                pltpu.make_async_remote_copy(
                    send_m.at[u, trow * 32 + tcol], recv_m.at[u, chip],
                    sems_send.at[u, 2], sems_recv.at[u, 2],
                    device_id=(core * 4 + trow, tcol), device_id_type=MESH,
                ).start()

            return 0

        lax.fori_loop(0, 128, one, 0, unroll=UNROLL)

        @pl.when(core == half_r)
        def _():
            recv_m[u, chip] = send_m[u, lax.rem(row, 4) * 32 + col]

    def wait_messages(buffer, sem, short):
        @pl.when(short)
        def _():
            bytes_wait(buffer.at[pl.ds(0, 127)], sem)

        @pl.when(jnp.logical_not(short))
        def _():
            bytes_wait(buffer, sem)

    def share_right(u):
        bytes_wait(recv_r.at[u, pl.ds(0, 127)], sems_recv.at[u, 0])
        mine = pl.ds(core * 128, 128)
        copy = pltpu.make_async_remote_copy(
            recv_r.at[u, mine], recv_r.at[u, mine], sems_send.at[u, 3], sems_recv.at[u, 3],
            device_id=(row, partner), device_id_type=MESH,
        )
        copy.start()
        return copy

    def woven(first, second):
        first, second = first.astype(F32), second.astype(F32)
        lane = lax.broadcasted_iota(jnp.int32, first.shape, 2)
        low_half = jnp.where(lane < 64, first, pltpu.roll(second, 64, 2))
        high_half = jnp.where(lane < 64, pltpu.roll(first, 64, 2), second)
        return jnp.concatenate([low_half, high_half], axis=1)

    def arrange_right(u):
        for par in range(2):
            for p in range(4):
                base = (par * 8 + 2 * p) * 16
                block = woven(recv_r[u, base : base + 16], recv_r[u, base + 16 : base + 32])
                if u == 0:
                    a_rt[p * 128 : (p + 1) * 128, par * 256 : (par + 1) * 256] = jnp.transpose(
                        block.reshape(256, 128)
                    ).astype(BF16)
                else:
                    a_r[:, par, :, p * 128 : (p + 1) * 128] = block.astype(BF16)

    def arrange_left(u):
        for par in range(2):
            if u == 0:
                for p in range(2):
                    base = (par * 4 + 2 * p) * 16
                    a_l0[par, :, :, p * 128 : (p + 1) * 128] = woven(
                        recv_l[u, base : base + 16], recv_l[u, base + 16 : base + 32]
                    ).astype(BF16)
            else:
                for p in range(4):
                    base = (par * 8 + 2 * p) * 8
                    a_l1[:, par, :, p * 128 : (p + 1) * 128] = woven(
                        recv_l[u, base : base + 8], recv_l[u, base + 8 : base + 16]
                    ).astype(BF16)

    def contract(u):
        for m in range(4):
            if u == 0:
                mixed = jnp.dot(
                    a_rt[128 * m : 128 * m + 128, :],
                    a_l0[...].reshape(512, 256),
                    preferred_element_type=F32,
                )
            else:
                mixed = lax.dot_general(
                    a_r[4 * m : 4 * m + 4].reshape(128, 512),
                    a_l1[...].reshape(256, 512),
                    (((1,), (1,)), ((), ())),
                    preferred_element_type=F32,
                )
            for p in range(2):
                both = mixed[:, p * 128 : (p + 1) * 128].reshape(8, 2, 8, 128)
                low_rows, high_rows = both[:, 0], both[:, 1]
                lane = lax.broadcasted_iota(jnp.int32, low_rows.shape, 2)
                start = 64 * p + 8 * m
                send_m[u, start : start + 8] = jnp.where(
                    lane < 64, low_rows, pltpu.roll(high_rows, 64, 2)
                ).astype(BF16)
                send_m[u, start + 32 : start + 40] = jnp.where(
                    lane < 64, pltpu.roll(low_rows, 64, 2), high_rows
                ).astype(BF16)

    def widen_mixed(u):
        def put(n, _):
            tmp_m[pl.ds(n * 128, 128), :] = (
                recv_m[u, pl.ds(n * 16, 16)].astype(F32).reshape(128, 128)
            )
            return 0

        lax.fori_loop(0, 8, put, 0, unroll=True)

    def finish(u, n):
        values = jnp.concatenate(
            [tmp_m[pl.ds(2 * n + k, 128, stride=8), :] for k in range(2)], axis=1
        )
        middle = norm_channels(values, mgain_t[u], mbias_t[u])
        outcome = jnp.dot(ow_t[u], middle, preferred_element_type=F32) + twice(obias_t[u])
        return state[n] + gates[n] * outcome

    def exchange(u, half, cover):
        send_right(u, 0)
        project(u, 0, tmp_l, send_l)
        send_left(u, half, 0)
        send_right(u, 1)
        send_left(u, half, 1)
        open_gates(u)
        cover()
        shared = share_right(u)
        shared.wait_recv()
        arrange_right(u)
        wait_messages(recv_l.at[u], sems_recv.at[u, 1], core == half)
        arrange_left(u)
        contract(u)
        send_mixed(u)
        wait_messages(recv_m.at[u], sems_recv.at[u, 2], core == half_r)
        widen_mixed(u)
        return shared

    def meet():
        pl.semaphore_wait(barrier, 38)

        def greet_again(t, _):
            pl.semaphore_signal(
                sem_enter, inc=1, device_id=(lax.rem(row + t, 8), col), device_id_type=MESH
            )
            return 0

        lax.fori_loop(1, 8, greet_again, 0)

    for load in loads:
        load.wait()
    prepare_projection(0)

    for n in range(4):
        blocks = [
            jnp.concatenate(
                [pair_ref[pl.ds(s, 64, stride=16), :], pair_ref[pl.ds(s + 8, 64, stride=16), :]],
                axis=0,
            )
            for s in (2 * n, 2 * n + 1)
        ]
        values = jnp.concatenate([jnp.transpose(block) for block in blocks], axis=1)
        state[n] = values
        normalise(0, n, values)
    meet()
    project(0, 256, tmp_r, send_r)

    pl.semaphore_wait(sem_enter, 7)

    def cover():
        prepare_finish(0)
        prepare_projection(1)
        prepare_finish(1)

    shared0 = exchange(0, half_r, cover)

    for n in range(4):
        values = finish(0, n)
        state[n] = values
        normalise(1, n, values)
    project(1, 256, tmp_r, send_r)

    shared1 = exchange(1, half_z, lambda: None)

    for n in range(4):
        values = finish(1, n)
        for k in range(2):
            s = 2 * n + k
            block = jnp.transpose(values[:, 128 * k : 128 * k + 128])
            out_ref[pl.ds(s, 64, stride=16), :] = block[0:64]
            out_ref[pl.ds(s + 8, 64, stride=16), :] = block[64:128]

    for u, shared, half in ((0, shared0, half_r), (1, shared1, half_z)):
        shared.wait_send()
        bytes_wait(send_r.at[u, pl.ds(0, 127)], sems_send.at[u, 0])
        wait_messages(send_l.at[u], sems_send.at[u, 1], core == half)
        wait_messages(send_m.at[u], sems_send.at[u, 2], core == half_r)


def body(pair, in_gain, in_bias, proj_weight, proj_bias, mid_gain, mid_bias, out_weight, out_bias):
    vmem = pl.BlockSpec(memory_space=pltpu.VMEM)
    out = pl.pallas_call(
        kernel,
        out_shape=jax.ShapeDtypeStruct((1024, 128), F32),
        in_specs=[pl.BlockSpec(memory_space=pltpu.HBM)] * 9,
        out_specs=vmem,
        scratch_shapes=[
            pltpu.VMEM((1024, 128), F32),
            pltpu.VMEM((2, 128), F32),
            pltpu.VMEM((2, 128), F32),
            pltpu.VMEM((2, 128, 640), BF16),
            pltpu.VMEM((2, 640), F32),
            pltpu.VMEM((2, 128), F32),
            pltpu.VMEM((2, 128), F32),
            pltpu.VMEM((2, 128, 128), BF16),
            pltpu.VMEM((2, 128), F32),
            pltpu.SemaphoreType.DMA((9,)),
            pltpu.VMEM((2, 640, 128), BF16),
            pltpu.VMEM((2, 128, 128), BF16),
            pltpu.VMEM((2, 640, 128), F32),
            pltpu.VMEM((2, 128, 128), F32),
            pltpu.VMEM((2, 128, 128), F32),
            pltpu.VMEM((2, 128, 128), F32),
            pltpu.VMEM((2, 128, 128), F32),
            pltpu.VMEM((2, 128, 128), F32),
            pltpu.VMEM((4, 128, 256), F32),
            pltpu.VMEM((4, 128, 256), F32),
            pltpu.VMEM((1024, 128), F32),
            pltpu.VMEM((1024, 128), F32),
            pltpu.VMEM((1024, 128), F32),
            pltpu.VMEM((2, 128, 8, 128), BF16),
            pltpu.VMEM((2, 128, 8, 128), BF16),
            pltpu.VMEM((2, 128, 8, 128), BF16),
            pltpu.VMEM((2, 128, 8, 128), BF16),
            pltpu.VMEM((2, 256, 8, 128), BF16),
            pltpu.VMEM((2, 128, 8, 128), BF16),
            pltpu.VMEM((2, 16, 16, 256), BF16),
            pltpu.VMEM((8, 2, 16, 512), BF16),
            pltpu.VMEM((16, 2, 16, 512), BF16),
            pltpu.VMEM((512, 512), BF16),
            pltpu.VMEM((4, 128, 256), BF16),
            pltpu.SemaphoreType.DMA((2, 4)),
            pltpu.SemaphoreType.DMA((2, 4)),
            pltpu.SemaphoreType.REGULAR,
        ],
        compiler_params=pltpu.CompilerParams(
            collective_id=0, has_side_effects=True
        ),
    )(
        pair.reshape(1024, 128), in_gain, in_bias, proj_weight, proj_bias,
        mid_gain, mid_bias, out_weight, out_bias,
    )
    return out.reshape(64, 16, 128)


def solution(mesh):
    placed = (P("row", "col", None), P(), P(), P(), P(), P(), P(), P(), P())
    return jax.shard_map(
        body, mesh=mesh, in_specs=placed, out_specs=P("row", "col", None), check_vma=False
    )
```

```python
import functools

import jax
import jax.numpy as jnp
from jax import lax
from jax.experimental import pallas as pl
from jax.experimental.pallas import tpu as pltpu
from jax.sharding import PartitionSpec as P

MESH = pl.DeviceIdType.MESH
F32 = jnp.float32
BF16 = jnp.bfloat16
EPS = 1e-05
UNROLL = 8


def twice(column):
    return jnp.concatenate([column, column], axis=1)


def norm_channels(values, gain, offset):
    mean = jnp.mean(values, 0, keepdims=True)
    centred = values - mean
    variance = jnp.mean(centred * centred, 0, keepdims=True)
    return (centred * lax.rsqrt(variance + EPS) * twice(gain) + twice(offset)).astype(BF16)


def kernel(
    pair_in, in_gain_in, in_bias_in, proj_w_in, proj_b_in, mid_gain_in, mid_bias_in,
    out_w_in, out_b_in,
    out_ref,
    pair_ref, in_gain, in_bias, proj_w, proj_b, mid_gain, mid_bias, out_w, out_b, sems_in,
    w_t, ow_t, bias_t, igain_t, ibias_t, mgain_t, mbias_t, obias_t,
    state, gates, tmp_l, tmp_r, tmp_m,
    send_l, send_r, send_m, recv_l, recv_r, recv_m,
    a_l0, a_l1, a_r, a_rt, normed,
    sems_send, sems_recv, sem_enter,
):
    row = lax.axis_index("row")
    col = lax.axis_index("col")
    y, xh = lax.div(row, 2), lax.rem(row, 2)
    z, low = lax.div(col, 4), lax.rem(col, 4)
    xl, core = lax.div(low, 2), lax.rem(low, 2)
    x = xh * 2 + xl
    chip = (y * 4 + x) * 8 + z
    partner = col + 1 - 2 * core
    half_r = lax.div(y, 2)
    half_z = lax.div(z, 4)

    barrier = pltpu.get_barrier_semaphore()

    def greet_row(t, _):
        pl.semaphore_signal(
            barrier, inc=1, device_id=(lax.rem(row + t, 8), col), device_id_type=MESH
        )
        return 0

    def greet_col(t, _):
        pl.semaphore_signal(
            barrier, inc=1, device_id=(row, lax.rem(col + t, 32)), device_id_type=MESH
        )
        return 0

    lax.fori_loop(1, 8, greet_row, 0)
    lax.fori_loop(1, 32, greet_col, 0)

    loads = [
        pltpu.make_async_copy(source, held, sems_in.at[n])
        for n, (source, held) in enumerate(
            (
                (proj_w_in, proj_w), (proj_b_in, proj_b), (mid_gain_in, mid_gain),
                (mid_bias_in, mid_bias), (in_gain_in, in_gain), (in_bias_in, in_bias),
                (pair_in, pair_ref), (out_w_in, out_w), (out_b_in, out_b),
            )
        )
    ]
    for load in loads:
        load.start()

    def column(held, u):
        return jnp.transpose(jnp.broadcast_to(held[u : u + 1, :], (128, held.shape[1])))

    def prepare_projection(u):
        w_t[u] = jnp.transpose(proj_w[u].astype(F32)).astype(BF16)
        igain_t[u] = column(in_gain, u)
        ibias_t[u] = column(in_bias, u)
        bias_t[u] = column(proj_b, u)

    def prepare_finish(u):
        ow_t[u] = jnp.transpose(out_w[u].astype(F32)).astype(BF16)
        mgain_t[u] = column(mid_gain, u)
        mbias_t[u] = column(mid_bias, u)
        obias_t[u] = column(out_b, u)

    def normalise(u, n, values):
        normed[n] = norm_channels(values, igain_t[u], ibias_t[u])

    def part(u, n, first):
        return jnp.dot(
            w_t[u, first : first + 128, :], normed[n], preferred_element_type=F32
        ) + twice(bias_t[u, first : first + 128, :])

    def project(u, first, held, packed):
        for n in range(4):
            values = jax.nn.sigmoid(part(u, n, first + 128)) * part(u, n, first)
            for k in range(2):
                held[pl.ds(2 * n + k, 128, stride=8), :] = values[:, 128 * k : 128 * k + 128]
        for n in range(8):
            packed[u, 16 * n : 16 * n + 16] = (
                held[128 * n : 128 * n + 128, :].reshape(16, 8, 128).astype(BF16)
            )

    def open_gates(u):
        for n in range(4):
            gates[n] = jax.nn.sigmoid(part(u, n, 512))

    def place(tx, ty, tz):
        there = (ty * 4 + tx) * 8 + tz
        return there, ty * 2 + lax.div(tx, 2), tz * 4 + lax.rem(tx, 2) * 2

    def far(n, size):
        return lax.select(
            lax.rem(n, 2) == 1, size // 2 - lax.div(n + 1, 2), size // 2 + lax.div(n, 2)
        )

    def target(t):
        part, rest = lax.div(t, 64), lax.rem(t, 64)
        tz = lax.rem(z + far(lax.rem(rest, 8), 8), 8)
        tx = lax.rem(x + far(lax.rem(lax.div(rest, 8), 4), 4), 4)
        ty = 2 * lax.rem(lax.div(y, 2) + 1 - lax.div(rest, 32), 2) + lax.rem(part + tx + tz, 2)
        return place(tx, ty, tz)

    def bytes_wait(buffer, sem):
        pltpu.make_async_copy(buffer, buffer, sem).wait()

    def send_right(u, part):
        slot = (core * 8 + row) * 16 + lax.div(col, 2)

        def one(t, _):
            there, trow, tcol = target(t)

            @pl.when(there != chip)
            def _():
                pltpu.make_async_remote_copy(
                    send_r.at[u, there], recv_r.at[u, slot],
                    sems_send.at[u, 0], sems_recv.at[u, 0],
                    device_id=(trow, tcol + core), device_id_type=MESH,
                ).start()

            return 0

        lax.fori_loop(64 * part, 64 * part + 64, one, 0, unroll=UNROLL)
        if part == 1:
            recv_r[u, slot] = send_r[u, chip]

    def send_left(u, half, part):
        if u == 0:
            slot = (core * 4 + lax.rem(row, 4)) * 16 + lax.div(col, 2)
        else:
            slot = (core * 8 + row) * 8 + lax.rem(lax.div(col, 2), 8)

        def one(t, _):
            there, trow, tcol = target(t)

            @pl.when(jnp.logical_or(there != chip, core != half))
            def _():
                pltpu.make_async_remote_copy(
                    send_l.at[u, there], recv_l.at[u, slot],
                    sems_send.at[u, 1], sems_recv.at[u, 1],
                    device_id=(trow, tcol + half), device_id_type=MESH,
                ).start()

            return 0

        lax.fori_loop(64 * part, 64 * part + 64, one, 0, unroll=UNROLL)
        if part == 1:

            @pl.when(core == half)
            def _():
                recv_l[u, slot] = send_l[u, chip]

    def send_mixed(u):
        def to(tz, tlow, trow):
            tcol = tz * 4 + tlow

            @pl.when(jnp.logical_or(core * 4 + trow != row, tcol != col))
            def _():
                pltpu.make_async_remote_copy(
                    send_m.at[u, trow * 32 + tcol], recv_m.at[u, chip],
                    sems_send.at[u, 2], sems_recv.at[u, 2],
                    device_id=(core * 4 + trow, tcol), device_id_type=MESH,
                ).start()

        def some(m, tcore):
            def one(t, _):
                tz = 2 * m + lax.div(t, 8 if u == 0 else 16)
                if u == 0:
                    rest = 7 - lax.rem(t, 8)
                    to(tz, lax.rem(xl + rest, 2) * 2 + tcore, lax.rem(row + lax.div(rest, 2), 4))
                else:
                    rest = 15 - lax.rem(t, 16)
                    to(tz, lax.rem(low + lax.rem(rest, 4), 4), lax.rem(row + lax.div(rest, 4), 4))
                return 0

            lax.fori_loop(0, 16 if u == 0 else 32, one, 0, unroll=UNROLL)

        blocks = [lax.rem(lax.div(z, 2) + ahead, 4) for ahead in (2, 1, 3, 0)]
        for n in range(4):
            contract(u, blocks[n])
        for n in range(4):
            some(blocks[n], 0)
        if u == 0:
            for n in range(4):
                some(blocks[n], 1)

        @pl.when(core == half_r)
        def _():
            recv_m[u, chip] = send_m[u, lax.rem(row, 4) * 32 + col]

    def wait_messages(buffer, sem, short):
        @pl.when(short)
        def _():
            bytes_wait(buffer.at[pl.ds(0, 127)], sem)

        @pl.when(jnp.logical_not(short))
        def _():
            bytes_wait(buffer, sem)

    def share_right(u):
        bytes_wait(recv_r.at[u, pl.ds(0, 127)], sems_recv.at[u, 0])
        mine = pl.ds(core * 128, 128)
        copy = pltpu.make_async_remote_copy(
            recv_r.at[u, mine], recv_r.at[u, mine], sems_send.at[u, 3], sems_recv.at[u, 3],
            device_id=(row, partner), device_id_type=MESH,
        )
        copy.start()
        return copy

    def woven(first, second):
        first, second = first.astype(F32), second.astype(F32)
        lane = lax.broadcasted_iota(jnp.int32, first.shape, 2)
        low_half = jnp.where(lane < 64, first, pltpu.roll(second, 64, 2))
        high_half = jnp.where(lane < 64, pltpu.roll(first, 64, 2), second)
        return jnp.concatenate([low_half, high_half], axis=1)

    def arrange_right(u):
        for par in range(2):
            for p in range(4):
                base = (par * 8 + 2 * p) * 16
                block = woven(recv_r[u, base : base + 16], recv_r[u, base + 16 : base + 32])
                if u == 0:
                    a_rt[p * 128 : (p + 1) * 128, par * 256 : (par + 1) * 256] = jnp.transpose(
                        block.reshape(256, 128)
                    ).astype(BF16)
                else:
                    a_r[:, par, :, p * 128 : (p + 1) * 128] = block.astype(BF16)

    def arrange_left(u):
        for par in range(2):
            if u == 0:
                for p in range(2):
                    base = (par * 4 + 2 * p) * 16
                    a_l0[par, :, :, p * 128 : (p + 1) * 128] = woven(
                        recv_l[u, base : base + 16], recv_l[u, base + 16 : base + 32]
                    ).astype(BF16)
            else:
                for p in range(4):
                    base = (par * 8 + 2 * p) * 8
                    a_l1[:, par, :, p * 128 : (p + 1) * 128] = woven(
                        recv_l[u, base : base + 8], recv_l[u, base + 8 : base + 16]
                    ).astype(BF16)

    def contract(u, m):
        if u == 0:
            mixed = jnp.dot(
                a_rt[pl.ds(pl.multiple_of(128 * m, 128), 128), :],
                a_l0[...].reshape(512, 256),
                preferred_element_type=F32,
            )
        else:
            mixed = lax.dot_general(
                a_r[pl.ds(4 * m, 4)].reshape(128, 512),
                a_l1[...].reshape(256, 512),
                (((1,), (1,)), ((), ())),
                preferred_element_type=F32,
            )
        for p in range(2):
            both = mixed[:, p * 128 : (p + 1) * 128].reshape(8, 2, 8, 128)
            low_rows, high_rows = both[:, 0], both[:, 1]
            lane = lax.broadcasted_iota(jnp.int32, low_rows.shape, 2)
            start = 64 * p + 8 * m
            send_m[u, pl.ds(start, 8)] = jnp.where(
                lane < 64, low_rows, pltpu.roll(high_rows, 64, 2)
            ).astype(BF16)
            send_m[u, pl.ds(start + 32, 8)] = jnp.where(
                lane < 64, pltpu.roll(low_rows, 64, 2), high_rows
            ).astype(BF16)

    def widen_mixed(u):
        def put(n, _):
            tmp_m[pl.ds(n * 128, 128), :] = (
                recv_m[u, pl.ds(n * 16, 16)].astype(F32).reshape(128, 128)
            )
            return 0

        lax.fori_loop(0, 8, put, 0, unroll=True)

    def finish(u, n):
        values = jnp.concatenate(
            [tmp_m[pl.ds(2 * n + k, 128, stride=8), :] for k in range(2)], axis=1
        )
        middle = norm_channels(values, mgain_t[u], mbias_t[u])
        outcome = jnp.dot(ow_t[u], middle, preferred_element_type=F32) + twice(obias_t[u])
        return state[n] + gates[n] * outcome

    def exchange(u, half, cover):
        send_right(u, 0)
        project(u, 0, tmp_l, send_l)
        send_left(u, half, 0)
        send_right(u, 1)
        send_left(u, half, 1)
        open_gates(u)
        cover()
        shared = share_right(u)
        shared.wait_recv()
        arrange_right(u)
        wait_messages(recv_l.at[u], sems_recv.at[u, 1], core == half)
        arrange_left(u)
        send_mixed(u)
        wait_messages(recv_m.at[u], sems_recv.at[u, 2], core == half_r)
        widen_mixed(u)
        return shared

    def meet():
        pl.semaphore_wait(barrier, 38)

        def greet_again(t, _):
            pl.semaphore_signal(
                sem_enter, inc=1, device_id=(lax.rem(row + t, 8), col), device_id_type=MESH
            )
            return 0

        lax.fori_loop(1, 8, greet_again, 0)

    for load in loads:
        load.wait()
    prepare_projection(0)

    for n in range(4):
        blocks = [
            jnp.concatenate(
                [pair_ref[pl.ds(s, 64, stride=16), :], pair_ref[pl.ds(s + 8, 64, stride=16), :]],
                axis=0,
            )
            for s in (2 * n, 2 * n + 1)
        ]
        values = jnp.concatenate([jnp.transpose(block) for block in blocks], axis=1)
        state[n] = values
        normalise(0, n, values)
    meet()
    project(0, 256, tmp_r, send_r)

    pl.semaphore_wait(sem_enter, 7)

    def cover():
        prepare_finish(0)
        prepare_projection(1)
        prepare_finish(1)

    shared0 = exchange(0, half_r, cover)

    for n in range(4):
        values = finish(0, n)
        state[n] = values
        normalise(1, n, values)
    project(1, 256, tmp_r, send_r)

    shared1 = exchange(1, half_z, lambda: None)

    for n in range(4):
        values = finish(1, n)
        for k in range(2):
            s = 2 * n + k
            block = jnp.transpose(values[:, 128 * k : 128 * k + 128])
            out_ref[pl.ds(s, 64, stride=16), :] = block[0:64]
            out_ref[pl.ds(s + 8, 64, stride=16), :] = block[64:128]

    for u, shared, half in ((0, shared0, half_r), (1, shared1, half_z)):
        shared.wait_send()
        bytes_wait(send_r.at[u, pl.ds(0, 127)], sems_send.at[u, 0])
        wait_messages(send_l.at[u], sems_send.at[u, 1], core == half)
        wait_messages(send_m.at[u], sems_send.at[u, 2], core == half_r)


def body(pair, in_gain, in_bias, proj_weight, proj_bias, mid_gain, mid_bias, out_weight, out_bias):
    vmem = pl.BlockSpec(memory_space=pltpu.VMEM)
    out = pl.pallas_call(
        kernel,
        out_shape=jax.ShapeDtypeStruct((1024, 128), F32),
        in_specs=[pl.BlockSpec(memory_space=pltpu.HBM)] * 9,
        out_specs=vmem,
        scratch_shapes=[
            pltpu.VMEM((1024, 128), F32),
            pltpu.VMEM((2, 128), F32),
            pltpu.VMEM((2, 128), F32),
            pltpu.VMEM((2, 128, 640), BF16),
            pltpu.VMEM((2, 640), F32),
            pltpu.VMEM((2, 128), F32),
            pltpu.VMEM((2, 128), F32),
            pltpu.VMEM((2, 128, 128), BF16),
            pltpu.VMEM((2, 128), F32),
            pltpu.SemaphoreType.DMA((9,)),
            pltpu.VMEM((2, 640, 128), BF16),
            pltpu.VMEM((2, 128, 128), BF16),
            pltpu.VMEM((2, 640, 128), F32),
            pltpu.VMEM((2, 128, 128), F32),
            pltpu.VMEM((2, 128, 128), F32),
            pltpu.VMEM((2, 128, 128), F32),
            pltpu.VMEM((2, 128, 128), F32),
            pltpu.VMEM((2, 128, 128), F32),
            pltpu.VMEM((4, 128, 256), F32),
            pltpu.VMEM((4, 128, 256), F32),
            pltpu.VMEM((1024, 128), F32),
            pltpu.VMEM((1024, 128), F32),
            pltpu.VMEM((1024, 128), F32),
            pltpu.VMEM((2, 128, 8, 128), BF16),
            pltpu.VMEM((2, 128, 8, 128), BF16),
            pltpu.VMEM((2, 128, 8, 128), BF16),
            pltpu.VMEM((2, 128, 8, 128), BF16),
            pltpu.VMEM((2, 256, 8, 128), BF16),
            pltpu.VMEM((2, 128, 8, 128), BF16),
            pltpu.VMEM((2, 16, 16, 256), BF16),
            pltpu.VMEM((8, 2, 16, 512), BF16),
            pltpu.VMEM((16, 2, 16, 512), BF16),
            pltpu.VMEM((512, 512), BF16),
            pltpu.VMEM((4, 128, 256), BF16),
            pltpu.SemaphoreType.DMA((2, 4)),
            pltpu.SemaphoreType.DMA((2, 4)),
            pltpu.SemaphoreType.REGULAR,
        ],
        compiler_params=pltpu.CompilerParams(
            collective_id=0, has_side_effects=True
        ),
    )(
        pair.reshape(1024, 128), in_gain, in_bias, proj_weight, proj_bias,
        mid_gain, mid_bias, out_weight, out_bias,
    )
    return out.reshape(64, 16, 128)


def solution(mesh):
    placed = (P("row", "col", None), P(), P(), P(), P(), P(), P(), P(), P())
    return jax.shard_map(
        body, mesh=mesh, in_specs=placed, out_specs=P("row", "col", None), check_vma=False
    )
```

```python
import functools

import jax
import jax.numpy as jnp
from jax import lax
from jax.experimental import pallas as pl
from jax.experimental.pallas import tpu as pltpu
from jax.sharding import PartitionSpec as P

MESH = pl.DeviceIdType.MESH
F32 = jnp.float32
BF16 = jnp.bfloat16
EPS = 1e-05
UNROLL = 8


def twice(column):
    return jnp.concatenate([column, column], axis=1)


def norm_channels(values, gain, offset):
    mean = jnp.mean(values, 0, keepdims=True)
    centred = values - mean
    variance = jnp.mean(centred * centred, 0, keepdims=True)
    return (centred * lax.rsqrt(variance + EPS) * twice(gain) + twice(offset)).astype(BF16)


def kernel(
    pair_in, in_gain_in, in_bias_in, proj_w_in, proj_b_in, mid_gain_in, mid_bias_in,
    out_w_in, out_b_in,
    out_ref,
    pair_ref, in_gain, in_bias, proj_w, proj_b, mid_gain, mid_bias, out_w, out_b, sems_in,
    w_t, ow_t, bias_t, igain_t, ibias_t, mgain_t, mbias_t, obias_t,
    state, gates, tmp_l, tmp_r, tmp_m,
    send_l, send_r, send_m, recv_l, recv_r, recv_m,
    a_l0, a_l1, a_r, a_rt, normed,
    sems_send, sems_recv, sem_enter,
):
    row = lax.axis_index("row")
    col = lax.axis_index("col")
    y, xh = lax.div(row, 2), lax.rem(row, 2)
    z, low = lax.div(col, 4), lax.rem(col, 4)
    xl, core = lax.div(low, 2), lax.rem(low, 2)
    x = xh * 2 + xl
    chip = (y * 4 + x) * 8 + z
    partner = col + 1 - 2 * core
    half_r = lax.div(y, 2)
    half_z = lax.div(z, 4)

    barrier = pltpu.get_barrier_semaphore()

    def greet_row(t, _):
        pl.semaphore_signal(
            barrier, inc=1, device_id=(lax.rem(row + t, 8), col), device_id_type=MESH
        )
        return 0

    def greet_col(t, _):
        pl.semaphore_signal(
            barrier, inc=1, device_id=(row, lax.rem(col + t, 32)), device_id_type=MESH
        )
        return 0

    lax.fori_loop(1, 8, greet_row, 0)
    lax.fori_loop(1, 32, greet_col, 0)

    loads = [
        pltpu.make_async_copy(source, held, sems_in.at[n])
        for n, (source, held) in enumerate(
            (
                (proj_w_in, proj_w), (proj_b_in, proj_b), (mid_gain_in, mid_gain),
                (mid_bias_in, mid_bias), (in_gain_in, in_gain), (in_bias_in, in_bias),
                (pair_in, pair_ref), (out_w_in, out_w), (out_b_in, out_b),
            )
        )
    ]
    for load in loads:
        load.start()

    def column(held, u):
        return jnp.transpose(jnp.broadcast_to(held[u : u + 1, :], (128, held.shape[1])))

    def prepare_projection(u):
        w_t[u] = jnp.transpose(proj_w[u].astype(F32)).astype(BF16)
        igain_t[u] = column(in_gain, u)
        ibias_t[u] = column(in_bias, u)
        bias_t[u] = column(proj_b, u)

    def prepare_finish(u):
        ow_t[u] = jnp.transpose(out_w[u].astype(F32)).astype(BF16)
        mgain_t[u] = column(mid_gain, u)
        mbias_t[u] = column(mid_bias, u)
        obias_t[u] = column(out_b, u)

    def normalise(u, n, values):
        normed[n] = norm_channels(values, igain_t[u], ibias_t[u])

    def part(u, n, first):
        return jnp.dot(
            w_t[u, first : first + 128, :], normed[n], preferred_element_type=F32
        ) + twice(bias_t[u, first : first + 128, :])

    def project(u, first, held, packed):
        for n in range(4):
            values = jax.nn.sigmoid(part(u, n, first + 128)) * part(u, n, first)
            for k in range(2):
                held[pl.ds(2 * n + k, 128, stride=8), :] = values[:, 128 * k : 128 * k + 128]
        for n in range(8):
            packed[u, 16 * n : 16 * n + 16] = (
                held[128 * n : 128 * n + 128, :].reshape(16, 8, 128).astype(BF16)
            )

    def open_gates(u):
        for n in range(4):
            gates[n] = jax.nn.sigmoid(part(u, n, 512))

    def place(tx, ty, tz):
        there = (ty * 4 + tx) * 8 + tz
        return there, ty * 2 + lax.div(tx, 2), tz * 4 + lax.rem(tx, 2) * 2

    def far(n, size):
        return lax.select(
            lax.rem(n, 2) == 1, size // 2 - lax.div(n + 1, 2), size // 2 + lax.div(n, 2)
        )

    def target(t):
        part, rest = lax.div(t, 64), lax.rem(t, 64)
        tz = lax.rem(z + far(lax.rem(rest, 8), 8), 8)
        tx = lax.rem(x + far(lax.rem(lax.div(rest, 8), 4), 4), 4)
        ty = 2 * lax.rem(lax.div(y, 2) + 1 - lax.div(rest, 32), 2) + lax.rem(part + tx + tz, 2)
        return place(tx, ty, tz)

    def bytes_wait(buffer, sem):
        pltpu.make_async_copy(buffer, buffer, sem).wait()

    def send_right(u, part):
        slot = (core * 8 + row) * 16 + lax.div(col, 2)

        def one(t, _):
            there, trow, tcol = target(t)

            @pl.when(there != chip)
            def _():
                pltpu.make_async_remote_copy(
                    send_r.at[u, there], recv_r.at[u, slot],
                    sems_send.at[u, 0], sems_recv.at[u, 0],
                    device_id=(trow, tcol + core), device_id_type=MESH,
                ).start()

            return 0

        lax.fori_loop(64 * part, 64 * part + 64, one, 0, unroll=UNROLL)
        if part == 1:
            recv_r[u, slot] = send_r[u, chip]

    def send_left(u, half, part):
        if u == 0:
            slot = (core * 4 + lax.rem(row, 4)) * 16 + lax.div(col, 2)
        else:
            slot = (core * 8 + row) * 8 + lax.rem(lax.div(col, 2), 8)

        def one(t, _):
            there, trow, tcol = target(t)

            @pl.when(jnp.logical_or(there != chip, core != half))
            def _():
                pltpu.make_async_remote_copy(
                    send_l.at[u, there], recv_l.at[u, slot],
                    sems_send.at[u, 1], sems_recv.at[u, 1],
                    device_id=(trow, tcol + half), device_id_type=MESH,
                ).start()

            return 0

        lax.fori_loop(64 * part, 64 * part + 64, one, 0, unroll=UNROLL)
        if part == 1:

            @pl.when(core == half)
            def _():
                recv_l[u, slot] = send_l[u, chip]

    def send_mixed(u):
        def to(tz, tlow, trow):
            tcol = tz * 4 + tlow

            @pl.when(jnp.logical_or(core * 4 + trow != row, tcol != col))
            def _():
                pltpu.make_async_remote_copy(
                    send_m.at[u, trow * 32 + tcol], recv_m.at[u, chip],
                    sems_send.at[u, 2], sems_recv.at[u, 2],
                    device_id=(core * 4 + trow, tcol), device_id_type=MESH,
                ).start()

        def some(first, second, tcore):
            def one(t, _):
                if second is None:
                    m = first
                else:
                    m = lax.select(lax.rem(t, 2) == 0, first, second)
                    t = lax.div(t, 2)
                tz = 2 * m + lax.div(t, 8 if u == 0 else 16)
                if u == 0:
                    rest = 7 - lax.rem(t, 8)
                    to(tz, lax.rem(xl + rest, 2) * 2 + tcore, lax.rem(row + lax.div(rest, 2), 4))
                else:
                    rest = 15 - lax.rem(t, 16)
                    to(tz, lax.rem(low + lax.rem(rest, 4), 4), lax.rem(row + lax.div(rest, 4), 4))
                return 0

            count = (16 if u == 0 else 32) * (1 if second is None else 2)
            lax.fori_loop(0, count, one, 0, unroll=UNROLL)

        def all_blocks(tcore):
            some(blocks[0], None, tcore)
            some(blocks[1], blocks[2], tcore)
            some(blocks[3], None, tcore)

        blocks = [lax.rem(lax.div(z, 2) + ahead, 4) for ahead in (2, 1, 3, 0)]
        for n in range(4):
            contract(u, blocks[n])
        all_blocks(0)
        if u == 0:
            all_blocks(1)

        @pl.when(core == half_r)
        def _():
            recv_m[u, chip] = send_m[u, lax.rem(row, 4) * 32 + col]

    def wait_messages(buffer, sem, short):
        @pl.when(short)
        def _():
            bytes_wait(buffer.at[pl.ds(0, 127)], sem)

        @pl.when(jnp.logical_not(short))
        def _():
            bytes_wait(buffer, sem)

    def share_right(u):
        bytes_wait(recv_r.at[u, pl.ds(0, 127)], sems_recv.at[u, 0])
        mine = pl.ds(core * 128, 128)
        copy = pltpu.make_async_remote_copy(
            recv_r.at[u, mine], recv_r.at[u, mine], sems_send.at[u, 3], sems_recv.at[u, 3],
            device_id=(row, partner), device_id_type=MESH,
        )
        copy.start()
        return copy

    def woven(first, second):
        first, second = first.astype(F32), second.astype(F32)
        lane = lax.broadcasted_iota(jnp.int32, first.shape, 2)
        low_half = jnp.where(lane < 64, first, pltpu.roll(second, 64, 2))
        high_half = jnp.where(lane < 64, pltpu.roll(first, 64, 2), second)
        return jnp.concatenate([low_half, high_half], axis=1)

    def arrange_right(u):
        for par in range(2):
            for p in range(4):
                base = (par * 8 + 2 * p) * 16
                block = woven(recv_r[u, base : base + 16], recv_r[u, base + 16 : base + 32])
                if u == 0:
                    a_rt[p * 128 : (p + 1) * 128, par * 256 : (par + 1) * 256] = jnp.transpose(
                        block.reshape(256, 128)
                    ).astype(BF16)
                else:
                    a_r[:, par, :, p * 128 : (p + 1) * 128] = block.astype(BF16)

    def arrange_left(u):
        for par in range(2):
            if u == 0:
                for p in range(2):
                    base = (par * 4 + 2 * p) * 16
                    a_l0[par, :, :, p * 128 : (p + 1) * 128] = woven(
                        recv_l[u, base : base + 16], recv_l[u, base + 16 : base + 32]
                    ).astype(BF16)
            else:
                for p in range(4):
                    base = (par * 8 + 2 * p) * 8
                    a_l1[:, par, :, p * 128 : (p + 1) * 128] = woven(
                        recv_l[u, base : base + 8], recv_l[u, base + 8 : base + 16]
                    ).astype(BF16)

    def contract(u, m):
        if u == 0:
            mixed = jnp.dot(
                a_rt[pl.ds(pl.multiple_of(128 * m, 128), 128), :],
                a_l0[...].reshape(512, 256),
                preferred_element_type=F32,
            )
        else:
            mixed = lax.dot_general(
                a_r[pl.ds(4 * m, 4)].reshape(128, 512),
                a_l1[...].reshape(256, 512),
                (((1,), (1,)), ((), ())),
                preferred_element_type=F32,
            )
        for p in range(2):
            both = mixed[:, p * 128 : (p + 1) * 128].reshape(8, 2, 8, 128)
            low_rows, high_rows = both[:, 0], both[:, 1]
            lane = lax.broadcasted_iota(jnp.int32, low_rows.shape, 2)
            start = 64 * p + 8 * m
            send_m[u, pl.ds(start, 8)] = jnp.where(
                lane < 64, low_rows, pltpu.roll(high_rows, 64, 2)
            ).astype(BF16)
            send_m[u, pl.ds(start + 32, 8)] = jnp.where(
                lane < 64, pltpu.roll(low_rows, 64, 2), high_rows
            ).astype(BF16)

    def widen_mixed(u):
        def put(n, _):
            tmp_m[pl.ds(n * 128, 128), :] = (
                recv_m[u, pl.ds(n * 16, 16)].astype(F32).reshape(128, 128)
            )
            return 0

        lax.fori_loop(0, 8, put, 0, unroll=True)

    def finish(u, n):
        values = jnp.concatenate(
            [tmp_m[pl.ds(2 * n + k, 128, stride=8), :] for k in range(2)], axis=1
        )
        middle = norm_channels(values, mgain_t[u], mbias_t[u])
        outcome = jnp.dot(ow_t[u], middle, preferred_element_type=F32) + twice(obias_t[u])
        return state[n] + gates[n] * outcome

    def exchange(u, half, cover):
        send_right(u, 0)
        project(u, 0, tmp_l, send_l)
        send_left(u, half, 0)
        send_right(u, 1)
        send_left(u, half, 1)
        open_gates(u)
        cover()
        shared = share_right(u)
        shared.wait_recv()
        arrange_right(u)
        wait_messages(recv_l.at[u], sems_recv.at[u, 1], core == half)
        arrange_left(u)
        send_mixed(u)
        wait_messages(recv_m.at[u], sems_recv.at[u, 2], core == half_r)
        widen_mixed(u)
        return shared

    def meet():
        pl.semaphore_wait(barrier, 38)

        def greet_again(t, _):
            pl.semaphore_signal(
                sem_enter, inc=1, device_id=(lax.rem(row + t, 8), col), device_id_type=MESH
            )
            return 0

        lax.fori_loop(1, 8, greet_again, 0)

    for load in loads:
        load.wait()
    prepare_projection(0)

    for n in range(4):
        blocks = [
            jnp.concatenate(
                [pair_ref[pl.ds(s, 64, stride=16), :], pair_ref[pl.ds(s + 8, 64, stride=16), :]],
                axis=0,
            )
            for s in (2 * n, 2 * n + 1)
        ]
        values = jnp.concatenate([jnp.transpose(block) for block in blocks], axis=1)
        state[n] = values
        normalise(0, n, values)
    meet()
    project(0, 256, tmp_r, send_r)

    pl.semaphore_wait(sem_enter, 7)

    def cover():
        prepare_finish(0)
        prepare_projection(1)
        prepare_finish(1)

    shared0 = exchange(0, half_r, cover)

    for n in range(4):
        values = finish(0, n)
        state[n] = values
        normalise(1, n, values)
    project(1, 256, tmp_r, send_r)

    shared1 = exchange(1, half_z, lambda: None)

    for n in range(4):
        values = finish(1, n)
        for k in range(2):
            s = 2 * n + k
            block = jnp.transpose(values[:, 128 * k : 128 * k + 128])
            out_ref[pl.ds(s, 64, stride=16), :] = block[0:64]
            out_ref[pl.ds(s + 8, 64, stride=16), :] = block[64:128]

    for u, shared, half in ((0, shared0, half_r), (1, shared1, half_z)):
        shared.wait_send()
        bytes_wait(send_r.at[u, pl.ds(0, 127)], sems_send.at[u, 0])
        wait_messages(send_l.at[u], sems_send.at[u, 1], core == half)
        wait_messages(send_m.at[u], sems_send.at[u, 2], core == half_r)


def body(pair, in_gain, in_bias, proj_weight, proj_bias, mid_gain, mid_bias, out_weight, out_bias):
    vmem = pl.BlockSpec(memory_space=pltpu.VMEM)
    out = pl.pallas_call(
        kernel,
        out_shape=jax.ShapeDtypeStruct((1024, 128), F32),
        in_specs=[pl.BlockSpec(memory_space=pltpu.HBM)] * 9,
        out_specs=vmem,
        scratch_shapes=[
            pltpu.VMEM((1024, 128), F32),
            pltpu.VMEM((2, 128), F32),
            pltpu.VMEM((2, 128), F32),
            pltpu.VMEM((2, 128, 640), BF16),
            pltpu.VMEM((2, 640), F32),
            pltpu.VMEM((2, 128), F32),
            pltpu.VMEM((2, 128), F32),
            pltpu.VMEM((2, 128, 128), BF16),
            pltpu.VMEM((2, 128), F32),
            pltpu.SemaphoreType.DMA((9,)),
            pltpu.VMEM((2, 640, 128), BF16),
            pltpu.VMEM((2, 128, 128), BF16),
            pltpu.VMEM((2, 640, 128), F32),
            pltpu.VMEM((2, 128, 128), F32),
            pltpu.VMEM((2, 128, 128), F32),
            pltpu.VMEM((2, 128, 128), F32),
            pltpu.VMEM((2, 128, 128), F32),
            pltpu.VMEM((2, 128, 128), F32),
            pltpu.VMEM((4, 128, 256), F32),
            pltpu.VMEM((4, 128, 256), F32),
            pltpu.VMEM((1024, 128), F32),
            pltpu.VMEM((1024, 128), F32),
            pltpu.VMEM((1024, 128), F32),
            pltpu.VMEM((2, 128, 8, 128), BF16),
            pltpu.VMEM((2, 128, 8, 128), BF16),
            pltpu.VMEM((2, 128, 8, 128), BF16),
            pltpu.VMEM((2, 128, 8, 128), BF16),
            pltpu.VMEM((2, 256, 8, 128), BF16),
            pltpu.VMEM((2, 128, 8, 128), BF16),
            pltpu.VMEM((2, 16, 16, 256), BF16),
            pltpu.VMEM((8, 2, 16, 512), BF16),
            pltpu.VMEM((16, 2, 16, 512), BF16),
            pltpu.VMEM((512, 512), BF16),
            pltpu.VMEM((4, 128, 256), BF16),
            pltpu.SemaphoreType.DMA((2, 4)),
            pltpu.SemaphoreType.DMA((2, 4)),
            pltpu.SemaphoreType.REGULAR,
        ],
        compiler_params=pltpu.CompilerParams(
            collective_id=0, has_side_effects=True
        ),
    )(
        pair.reshape(1024, 128), in_gain, in_bias, proj_weight, proj_bias,
        mid_gain, mid_bias, out_weight, out_bias,
    )
    return out.reshape(64, 16, 128)


def solution(mesh):
    placed = (P("row", "col", None), P(), P(), P(), P(), P(), P(), P(), P())
    return jax.shard_map(
        body, mesh=mesh, in_specs=placed, out_specs=P("row", "col", None), check_vma=False
    )
```
